8 devices in a mesh: dp: 1 (over z), fsdp: 8 (over y, x, core).
Axes of the slice: x: 2, y: 2, z: 1, core: 2. Of those that a mesh axis runs over, the one named last changes fastest.
Arguments:
- tokens: bfloat16 [16, 512, 7168], P(('dp', 'fsdp'))
- gain_in: bfloat16 [7168], P('fsdp')
- w_dq: bfloat16 [7168, 1536], P('fsdp')
- gain_q: bfloat16 [1536], P('fsdp')
- w_uq: bfloat16 [1536, 12288], P('fsdp')
- w_dkv: bfloat16 [7168, 576], P('fsdp')
- gain_kv: bfloat16 [512], P('fsdp')
- w_ukv: bfloat16 [512, 16384], P('fsdp')
- w_out: bfloat16 [8192, 7168], P('fsdp')
Outputs:
- output 1: bfloat16 [16, 512, 7168], P(('dp', 'fsdp'))
- output 2: bfloat16 [16, 512, 512], P(('dp', 'fsdp'))
- output 3: bfloat16 [16, 512, 64], P(('dp', 'fsdp'))
All inputs are finite; a program needn't handle non-finite values.
Results may differ from the reference program's by a relative error of at most 0.00556248.
Values are sent between devices in bfloat16 or wider.
A program may use at most 1 GiB of HBM per device.

```python
import jax
import jax.numpy as jnp
from jax import lax

PROMPTS = 16
SEQ_LEN = 512
D_MODEL = 7168
N_HEADS = 64
Q_RANK = 1536
KV_RANK = 512
NOPE_DIM = 128
ROPE_DIM = 64
V_DIM = 128
EPSILON = 1e-6
ROPE_THETA = 10000.0


def setup_inputs(seed: int = 0, part: int = 0) -> dict:
    key_list = jax.random.split(jax.random.key(seed), 9)

    def draw_weight(sub_key, n_rows, n_cols):
        drawn = jax.random.normal(sub_key, (n_rows, n_cols), jnp.float32) * (n_rows ** -0.5)
        return drawn.astype(jnp.bfloat16)

    def draw_gain(sub_key, n_items, centre):
        drawn = centre * (1.0 + 0.3 * jax.random.normal(sub_key, (n_items,), jnp.float32))
        return drawn.astype(jnp.bfloat16)

    tok_key = jax.random.fold_in(key_list[0], part)
    tokens = jax.random.normal(tok_key, (PROMPTS, SEQ_LEN, D_MODEL), jnp.float32).astype(jnp.bfloat16)
    return {
        'tokens': tokens,
        'gain_in': draw_gain(key_list[1], D_MODEL, 1.0),
        'w_dq': draw_weight(key_list[2], D_MODEL, Q_RANK),
        'gain_q': draw_gain(key_list[3], Q_RANK, 2.0),
        'w_uq': draw_weight(key_list[4], Q_RANK, N_HEADS * (NOPE_DIM + ROPE_DIM)),
        'w_dkv': draw_weight(key_list[5], D_MODEL, KV_RANK + ROPE_DIM),
        'gain_kv': draw_gain(key_list[6], KV_RANK, 1.0),
        'w_ukv': draw_weight(key_list[7], KV_RANK, N_HEADS * (NOPE_DIM + V_DIM)),
        'w_out': draw_weight(key_list[8], N_HEADS * V_DIM, D_MODEL),
    }


def rms_scale(values_in, gain_vec):
    values_f32 = values_in.astype(jnp.float32)
    inv_rms = lax.rsqrt(jnp.mean(values_f32 * values_f32, axis=-1, keepdims=True) + EPSILON)
    return values_f32 * inv_rms * gain_vec.astype(jnp.float32)


def rope_tables():
    half_dim = ROPE_DIM // 2
    inv_freq = ROPE_THETA ** (-2.0 * jnp.arange(half_dim, dtype=jnp.float32) / ROPE_DIM)
    angles = jnp.arange(SEQ_LEN, dtype=jnp.float32)[:, None] * inv_freq[None, :]
    return jnp.cos(angles), jnp.sin(angles)


def apply_rope(values_in, cos_t, sin_t):
    half_dim = values_in.shape[-1] // 2
    lo_half = values_in[..., :half_dim]
    hi_half = values_in[..., half_dim:]
    return jnp.concatenate([lo_half * cos_t - hi_half * sin_t, hi_half * cos_t + lo_half * sin_t], axis=-1)


def one_prompt(tok_rows, gain_in, w_dq, gain_q, w_uq, w_dkv, gain_kv, w_ukv, w_out):
    cos_t, sin_t = rope_tables()
    normed = rms_scale(tok_rows, gain_in).astype(jnp.bfloat16)
    q_down = jnp.dot(normed, w_dq, preferred_element_type=jnp.float32)
    q_lat = rms_scale(q_down, gain_q).astype(jnp.bfloat16)
    q_full = jnp.dot(q_lat, w_uq, preferred_element_type=jnp.float32).reshape(SEQ_LEN, N_HEADS, NOPE_DIM + ROPE_DIM)
    q_nope = q_full[:, :, :NOPE_DIM].astype(jnp.bfloat16)
    q_pe = apply_rope(q_full[:, :, NOPE_DIM:], cos_t[:, None, :], sin_t[:, None, :]).astype(jnp.bfloat16)
    kv_down = jnp.dot(normed, w_dkv, preferred_element_type=jnp.float32)
    latent = rms_scale(kv_down[:, :KV_RANK], gain_kv).astype(jnp.bfloat16)
    k_pe = apply_rope(kv_down[:, KV_RANK:], cos_t, sin_t).astype(jnp.bfloat16)
    kv_up = jnp.dot(latent, w_ukv, preferred_element_type=jnp.float32).astype(jnp.bfloat16)
    kv_up = kv_up.reshape(SEQ_LEN, N_HEADS, NOPE_DIM + V_DIM)
    k_nope = kv_up[:, :, :NOPE_DIM].astype(jnp.float32)
    values = kv_up[:, :, NOPE_DIM:].astype(jnp.float32)
    score_scale = (NOPE_DIM + ROPE_DIM) ** -0.5
    scores = jnp.einsum('qhd,khd->hqk', q_nope.astype(jnp.float32), k_nope)
    scores = scores + jnp.einsum('qhd,kd->hqk', q_pe.astype(jnp.float32), k_pe.astype(jnp.float32))
    causal = jnp.arange(SEQ_LEN)[:, None] >= jnp.arange(SEQ_LEN)[None, :]
    scores = jnp.where(causal[None, :, :], scores * score_scale, -1e30)
    attn_probs = jax.nn.softmax(scores, axis=-1).astype(jnp.bfloat16)
    attn_out = jnp.einsum('hqk,khd->qhd', attn_probs.astype(jnp.float32), values).astype(jnp.bfloat16)
    attn_out = attn_out.reshape(SEQ_LEN, N_HEADS * V_DIM)
    proj_out = jnp.dot(attn_out, w_out, preferred_element_type=jnp.float32)
    y_rows = (tok_rows.astype(jnp.float32) + proj_out).astype(jnp.bfloat16)
    return y_rows, latent, k_pe


def reference(tokens, gain_in, w_dq, gain_q, w_uq, w_dkv, gain_kv, w_ukv, w_out):
    def per_prompt(tok_rows):
        return one_prompt(tok_rows, gain_in, w_dq, gain_q, w_uq, w_dkv, gain_kv, w_ukv, w_out)

    y_out, kv_cache, pe_cache = lax.map(per_prompt, tokens)
    return (y_out, kv_cache, pe_cache)
```

```python
import functools

import jax
import jax.numpy as jnp
import numpy as np
from jax import lax
from jax.experimental import pallas as pl
from jax.experimental.pallas import tpu as pltpu
from jax.sharding import PartitionSpec as P

EPSILON = 1e-6
ROPE_THETA = 10000.0
MESH = pl.DeviceIdType.MESH
F32 = jnp.float32
BF16 = jnp.bfloat16

RX, RY, RD, RP = 0, 1, 2, 3

N_DEV = 8
LOOKAHEAD = 3


def rope_consts(seq_len, rope_dim):
    half = rope_dim // 2
    inv_freq = (ROPE_THETA ** (-2.0 * np.arange(half, dtype=np.float32) / rope_dim)).astype(np.float32)
    angles = np.arange(seq_len, dtype=np.float32)[:, None] * inv_freq[None, :]
    cos_t = np.cos(angles).astype(np.float32)
    sin_t = np.sin(angles).astype(np.float32)
    cos2 = np.concatenate([cos_t, cos_t, cos_t, cos_t], axis=1)
    sin2 = np.concatenate([-sin_t, sin_t, -sin_t, sin_t], axis=1)
    return cos2, sin2


def rope128(v, cos2, sin2):
    lane = lax.broadcasted_iota(jnp.int32, v.shape, 1)
    swapped = jnp.where(lane % 64 < 32, pltpu.roll(v, 96, 1), pltpu.roll(v, 32, 1))
    return v * cos2 + swapped * sin2


def dot(a, b):
    return lax.dot_general(a, b, (((1,), (0,)), ((), ())), preferred_element_type=F32)


def dot_nt(a, b):
    return lax.dot_general(a, b, (((1,), (1,)), ((), ())), preferred_element_type=F32)


def block_kernel(
    cfg,
    x_hbm, gains_hbm, w_dq, w_uq, w_dkv, w_ukv, w_o, cos_hbm, sin_hbm,
    y_hbm, c_hbm, r_hbm, g_dq, g_uq, g_dkv, g_ukv, g_o,
    ao, qd, cq, c_s, r_lo, r_hi, r_out, cos_s, sin_s, gbuf, g1row, gqrow, gkvrow,
    wkv, wbig, wuq, wukv, q4, kv4, xres, yout,
    send_sem, recv_sem, load_sem, x_sem, y_sem, misc_sem, gain_send, gain_recv,
):
    tok = cfg["tok"]
    seq = cfg["seq"]
    width = cfg["width"]
    q_rank = cfg["q_rank"]
    kv_rank = cfg["kv_rank"]
    kdim = cfg["kdim"]
    n_dq, n_u, n_o = cfg["n_dq"], cfg["n_u"], cfg["n_o"]
    dq_w, o_w = cfg["dq_w"], cfg["o_w"]
    uq_w, ukv_w = cfg["uq_w"], cfg["ukv_w"]
    score_scale = cfg["score_scale"]
    first_u = 1 + n_dq
    first_o = first_u + n_u
    n_ticks = first_o + n_o

    me = lax.axis_index("fsdp")
    xn, yn, pt = me ^ 2, me ^ 4, me ^ 1

    def dev(t):
        return (lax.axis_index("dp"), t)

    barrier = pltpu.get_barrier_semaphore()
    for k in range(1, N_DEV):
        pl.semaphore_signal(barrier, inc=1, device_id=dev(me ^ k), device_id_type=MESH)
    pl.semaphore_wait(barrier, N_DEV - 1)

    gain_copies = []
    for k in range(1, N_DEV):
        gain_copies.append(pltpu.make_async_remote_copy(
            src_ref=gains_hbm.at[0], dst_ref=gbuf.at[me], send_sem=gain_send.at[k], recv_sem=gain_recv.at[k],
            device_id=dev(me ^ k), device_id_type=MESH))
        gain_copies[-1].start()

    class Piece:
        def __init__(self, local, full, n, cid, c0, w):
            self.local, self.full, self.n, self.cid = local, full, n, cid
            self.cols = pl.ds(pl.multiple_of(c0, 128), w)

        def shard(self, s, r0=0, nr=None):
            nr = self.n if nr is None else nr
            return self.full.at[pl.ds(pl.multiple_of(s * self.n + r0, 16), nr), self.cols]

        def remote(self, src, dst, k, t):
            return pltpu.make_async_remote_copy(
                src_ref=src, dst_ref=dst, send_sem=send_sem.at[self.cid], recv_sem=recv_sem.at[self.cid, k],
                device_id=dev(t), device_id_type=MESH)

        def send_own(self):
            for k, t in ((RX, xn), (RY, yn), (RP, pt)):
                self.remote(self.local.at[:, self.cols], self.shard(me), k, t).start()

        def on_xy(self):
            half = self.n // 2
            sx, sy = self.shard(xn), self.shard(yn)
            self.remote(sx, sx, RX, xn).wait_recv()
            s = self.shard(xn, 0, half)
            self.remote(s, s, RD, yn).start()
            self.remote(sx, sx, RP, pt).start()
            self.remote(sy, sy, RY, yn).wait_recv()
            s = self.shard(yn, half, half)
            self.remote(s, s, RD, xn).start()
            self.remote(sy, sy, RP, pt).start()

        def on_d(self):
            s = self.shard(me ^ 6)
            self.remote(s, s, RD, pt).wait_recv()
            self.remote(s, s, RP, pt).start()

        def on_p(self):
            s = self.full.at[pl.ds(0, 4 * self.n), self.cols]
            self.remote(s, s, RP, pt).wait_recv()

        def drain(self):
            s = self.full.at[pl.ds(0, 7 * self.n), self.cols]
            self.remote(s, s, RP, pt).wait_send()

        def load(self, buf, sem):
            for k in range(N_DEV):
                s = me ^ k
                src = self.local.at[:, self.cols] if k == 0 else self.shard(s)
                pltpu.make_async_copy(src, buf.at[pl.ds(pl.multiple_of(s * self.n, 16), self.n), :], sem).start()

        def wait_load(self, buf, sem):
            d = buf.at[pl.ds(0, N_DEV * self.n), :]
            pltpu.make_async_copy(d, d, sem).wait()

    def kv_pieces(_):
        return [Piece(w_dkv, g_dkv, w_dkv.shape[0], 0, 0, w_dkv.shape[1])]

    def dq_pieces(c):
        return [Piece(w_dq, g_dq, w_dq.shape[0], 1 + c, c * dq_w, dq_w)]

    def u_pieces(g):
        return [
            Piece(w_ukv, g_ukv, w_ukv.shape[0], first_u + 2 * g, g * ukv_w, ukv_w),
            Piece(w_uq, g_uq, w_uq.shape[0], first_u + 2 * g + 1, g * uq_w, uq_w),
        ]

    def o_pieces(n):
        return [Piece(w_o, g_o, w_o.shape[0], first_u + 2 * n_u + n, n * o_w, o_w)]

    def kv_bufs(_):
        return [(wkv, load_sem.at[4])]

    def dq_bufs(c):
        s = c % 2
        return [(wbig.at[s], load_sem.at[s])]

    def u_bufs(g):
        s = g % 2
        return [(wukv.at[s], load_sem.at[5 + s]), (wuq.at[s], load_sem.at[2 + s])]

    kinds = [
        (0, 1, kv_pieces, kv_bufs),
        (1, n_dq, dq_pieces, dq_bufs),
        (first_u, n_u, u_pieces, u_bufs),
        (first_o, n_o, o_pieces, dq_bufs),
    ]

    def each_kind(i, fn):
        for k, (first, count, _, _) in enumerate(kinds):
            @pl.when((i >= first) & (i < first + count))
            def _():
                fn(k, i - first)

    def send_own(k, c):
        for p in kinds[k][2](c):
            p.send_own()

    def on_xy(k, c):
        for p in kinds[k][2](c):
            p.on_xy()

    def arrive(k, c):
        for p in kinds[k][2](c):
            p.on_d()
        for p in kinds[k][2](c):
            p.on_p()
        if cfg["compute"]:
            for p, (buf, sem) in zip(kinds[k][2](c), kinds[k][3](c)):
                p.load(buf, sem)
            if k == 3:
                s = c % 2
                pltpu.make_async_copy(
                    x_hbm.at[:, pl.ds(pl.multiple_of(c * o_w, 128), o_w)], xres.at[s], x_sem.at[s]).start()

    mb = cfg["mb"]
    n_mb = tok // mb

    def compute_kv(_):
        def body(m, carry):
            rows = pl.ds(pl.multiple_of(m * mb, mb), mb)
            u = dot(ao[rows, 0:width], wkv[...])
            lat = u[:, 0:kv_rank]
            inv = lax.rsqrt(jnp.mean(lat * lat, axis=-1, keepdims=True) + EPSILON)
            c_s[rows, :] = (lat * inv * gkvrow[...]).astype(BF16)
            pe = jnp.concatenate([u[:, kv_rank:], jnp.zeros((mb, 64), F32)], axis=1)
            trows = pl.ds(pl.multiple_of((m * mb) % seq, mb), mb)
            rot = rope128(pe, cos_s[trows, :], sin_s[trows, :])
            r_lo[rows, :] = rot.astype(BF16)
            r_hi[rows, :] = pltpu.roll(rot, 64, 1).astype(BF16)
            r_out[rows, :] = rot[:, 0:64].astype(BF16)
            return carry

        lax.fori_loop(0, n_mb, body, 0)
        pltpu.make_async_copy(c_s, c_hbm, misc_sem.at[0]).start()
        pltpu.make_async_copy(r_out, r_hbm, misc_sem.at[1]).start()

    def compute_dq(c):
        slot = c % 2
        cols = pl.ds(pl.multiple_of(c * dq_w, 128), dq_w)

        def body(m, carry):
            rows = pl.ds(pl.multiple_of(m * mb, mb), mb)
            qd[rows, cols] = dot(ao[rows, 0:width], wbig[slot, 0:width, :])
            return carry

        lax.fori_loop(0, n_mb, body, 0)

        @pl.when(c == n_dq - 1)
        def _():
            def norm(m, carry):
                rows = pl.ds(pl.multiple_of(m * 32, 32), 32)
                v = qd[rows, :]
                inv = lax.rsqrt(jnp.mean(v * v, axis=-1, keepdims=True) + EPSILON)
                cq[rows, :] = (v * inv * gqrow[...]).astype(BF16)
                return carry

            lax.fori_loop(0, tok // 32, norm, 0)

    def compute_u(g):
        slot = g % 2

        def proj(m, carry):
            rows = pl.ds(pl.multiple_of(m * mb, mb), mb)
            trows = pl.ds(pl.multiple_of((m * mb) % seq, mb), mb)
            kv4[rows, :] = dot(c_s[rows, :], wukv[slot]).astype(BF16)
            q = dot(cq[rows, :], wuq[slot])
            cos2, sin2 = cos_s[trows, :], sin_s[trows, :]
            lane = lax.broadcasted_iota(jnp.int32, (mb, 128), 1)
            for p in range(uq_w // 384):
                b0 = q[:, 384 * p:384 * p + 128]
                b1 = q[:, 384 * p + 128:384 * p + 256]
                b2 = q[:, 384 * p + 256:384 * p + 384]
                q4[rows, 384 * p:384 * p + 128] = b0.astype(BF16)
                q4[rows, 384 * p + 128:384 * p + 256] = jnp.where(lane < 64, rope128(b1, cos2, sin2), b1).astype(BF16)
                q4[rows, 384 * p + 256:384 * p + 384] = jnp.where(lane < 64, b2, rope128(b2, cos2, sin2)).astype(BF16)
            return carry

        lax.fori_loop(0, n_mb, proj, 0)

        n_pairs = uq_w // 384
        qb_rows = 256

        def attn(t, carry):
            b, p = t // n_pairs, t % n_pairs
            brow = pl.multiple_of(b * seq, seq)
            rows = pl.ds(brow, seq)
            for hh in range(2):
                koff = pl.multiple_of(p * 512 + hh * 256, 128)
                k = kv4[rows, pl.ds(koff, 128)]
                v = kv4[rows, pl.ds(pl.multiple_of(koff + 128, 128), 128)]
                if hh == 0:
                    k_a, k_b = k, r_lo[rows, :]
                else:
                    lane = lax.broadcasted_iota(jnp.int32, (seq, 128), 1)
                    kr = pltpu.roll(k.astype(F32), 64, 1)
                    k_a = jnp.where(lane < 64, 0.0, kr).astype(BF16)
                    k_b = jnp.where(lane < 64, kr, r_hi[rows, :].astype(F32)).astype(BF16)
                kcat = jnp.concatenate([k_a, k_b], axis=1)
                for qb in range(seq // qb_rows):
                    nk = qb_rows * (qb + 1)
                    qrow = pl.ds(pl.multiple_of(brow + qb * qb_rows, qb_rows), qb_rows)
                    q = q4[qrow, pl.ds(pl.multiple_of(p * 384 + hh * 128, 128), 256)]
                    s = dot_nt(q, kcat[0:nk, :]) * (score_scale * 1.4426950408889634)
                    row = lax.broadcasted_iota(jnp.int32, (qb_rows, nk), 0) + qb * qb_rows
                    col = lax.broadcasted_iota(jnp.int32, (qb_rows, nk), 1)
                    s = jnp.where(row >= col, s, -1e30)
                    e = jnp.exp2(s - jnp.max(s, axis=-1, keepdims=True))
                    probs = (e * (1.0 / jnp.sum(e, axis=-1, keepdims=True))).astype(BF16)
                    o = dot(probs, v[0:nk, :])
                    ocol = pl.multiple_of((g * n_pairs * 2 + p * 2 + hh) * 128, 128)
                    ao[qrow, pl.ds(ocol, 128)] = o.astype(BF16)
            return carry

        lax.fori_loop(0, (tok // seq) * n_pairs, attn, 0)

    def y_copy(c, slot):
        return pltpu.make_async_copy(
            yout.at[slot], y_hbm.at[:, pl.ds(pl.multiple_of(c * o_w, 128), o_w)], y_sem.at[slot])

    def compute_o(c):
        slot = c % 2
        pltpu.make_async_copy(xres.at[slot], xres.at[slot], x_sem.at[slot]).wait()

        @pl.when(c >= 2)
        def _():
            y_copy(c - 2, slot).wait()

        def body(m, carry):
            rows = pl.ds(pl.multiple_of(m * mb, mb), mb)
            acc = dot(ao[rows, 0:kdim], wbig[slot])
            yout[slot, rows, :] = (xres[slot, rows, :].astype(F32) + acc).astype(BF16)
            return carry

        lax.fori_loop(0, n_mb, body, 0)
        y_copy(c, slot).start()

    def compute(k, c):
        for p, (buf, sem) in zip(kinds[k][2](c), kinds[k][3](c)):
            p.wait_load(buf, sem)
        (compute_kv, compute_dq, compute_u, compute_o)[k](c)

    for i in range(LOOKAHEAD):
        for k, (first, count, _, _) in enumerate(kinds):
            if first <= i < first + count:
                send_own(k, i - first)

    local = [
        pltpu.make_async_copy(gains_hbm.at[0], gbuf.at[me], misc_sem.at[2]),
        pltpu.make_async_copy(cos_hbm, cos_s, misc_sem.at[3]),
        pltpu.make_async_copy(sin_hbm, sin_s, misc_sem.at[4]),
        pltpu.make_async_copy(x_hbm, ao.at[:, pl.ds(0, width)], misc_sem.at[5]),
    ]
    for cp in local:
        cp.start()
    for cp in local:
        cp.wait()
    for k in range(1, N_DEV):
        gain_copies[k - 1].wait()

    n1, nq, nkv = width // N_DEV, q_rank // N_DEV, kv_rank // N_DEV
    for j in range(N_DEV):
        g1row[:, n1 * j:n1 * (j + 1)] = gbuf[j, :, 0:n1]
    gqrow[...] = jnp.concatenate([gbuf[j, :, n1:n1 + nq] for j in range(N_DEV)], axis=1)
    gkvrow[...] = jnp.concatenate([gbuf[j, :, n1 + nq:n1 + nq + nkv] for j in range(N_DEV)], axis=1)

    if cfg["compute"]:
        def norm_x(m, carry):
            rows = pl.ds(pl.multiple_of(m * 16, 16), 16)
            v = ao[rows, 0:width].astype(F32)
            inv = lax.rsqrt(jnp.mean(v * v, axis=-1, keepdims=True) + EPSILON)
            ao[rows, 0:width] = (v * inv * g1row[...]).astype(BF16)
            return carry

        lax.fori_loop(0, tok // 16, norm_x, 0)

    def tick(i, carry):
        each_kind(i, on_xy)
        each_kind(i + LOOKAHEAD, send_own)
        each_kind(i - 1, arrive)
        if cfg["compute"]:
            each_kind(i - 2, compute)
        return carry

    lax.fori_loop(0, n_ticks + 2, tick, 0)

    def drain(i, carry):
        each_kind(i, lambda k, c: [p.drain() for p in kinds[k][2](c)])
        return carry

    lax.fori_loop(0, n_ticks, drain, 0)
    if cfg["compute"]:
        pltpu.make_async_copy(c_s, c_hbm, misc_sem.at[0]).wait()
        pltpu.make_async_copy(r_out, r_hbm, misc_sem.at[1]).wait()
        y_copy(n_o - 2, (n_o - 2) % 2).wait()
        y_copy(n_o - 1, (n_o - 1) % 2).wait()


def solution(mesh, compute=True):
    batch_spec = P(("dp", "fsdp"))
    row_spec = P("fsdp")
    mat_spec = P("fsdp", None)

    def run_block(tokens, gain_in, w_dq, gain_q, w_uq, w_dkv, gain_kv, w_ukv, w_out):
        seq = tokens.shape[1]
        rope_dim = w_dkv.shape[1] - gain_kv.shape[0]
        nope_total = w_ukv.shape[1] - w_out.shape[0]
        n_heads = (w_uq.shape[1] - nope_total) // rope_dim
        cos2, sin2 = rope_consts(seq, rope_dim)

        def local_block(tok_blk, g1, wdq, gq, wuq, wdkv, gkv, wukv, wo):
            n_prompts, _, width = tok_blk.shape
            tok = n_prompts * seq
            q_rank, kv_rank = gain_q.shape[0], gain_kv.shape[0]
            heads_per = 4
            cfg = dict(
                tok=tok, seq=seq, width=width, q_rank=q_rank, kv_rank=kv_rank, kdim=w_out.shape[0],
                n_dq=q_rank // 256, n_u=n_heads // heads_per, n_o=width // 256, dq_w=256, o_w=256,
                uq_w=heads_per * (w_uq.shape[1] // n_heads), ukv_w=heads_per * (w_ukv.shape[1] // n_heads),
                score_scale=(w_uq.shape[1] // n_heads) ** -0.5, mb=256, compute=compute,
            )
            n_sems = 1 + cfg["n_dq"] + 2 * cfg["n_u"] + cfg["n_o"]
            gains = jnp.concatenate([g1, gq, gkv]).astype(F32).reshape(1, 1, -1)
            n_g = gains.shape[2]
            any_spec = pl.BlockSpec(memory_space=pl.ANY)
            outs = pl.pallas_call(
                functools.partial(block_kernel, cfg),
                out_shape=[
                    jax.ShapeDtypeStruct((tok, width), BF16),
                    jax.ShapeDtypeStruct((tok, kv_rank), BF16),
                    jax.ShapeDtypeStruct((tok, rope_dim), BF16),
                    jax.ShapeDtypeStruct(w_dq.shape, BF16),
                    jax.ShapeDtypeStruct(w_uq.shape, BF16),
                    jax.ShapeDtypeStruct(w_dkv.shape, BF16),
                    jax.ShapeDtypeStruct(w_ukv.shape, BF16),
                    jax.ShapeDtypeStruct(w_out.shape, BF16),
                ],
                in_specs=[any_spec] * 9,
                out_specs=[any_spec] * 8,
                scratch_shapes=[
                    pltpu.VMEM((tok, cfg["kdim"]), BF16),
                    pltpu.VMEM((tok, q_rank), F32),
                    pltpu.VMEM((tok, q_rank), BF16),
                    pltpu.VMEM((tok, kv_rank), BF16),
                    pltpu.VMEM((tok, 128), BF16),
                    pltpu.VMEM((tok, 128), BF16),
                    pltpu.VMEM((tok, rope_dim), BF16),
                    pltpu.VMEM((seq, 128), F32),
                    pltpu.VMEM((seq, 128), F32),
                    pltpu.VMEM((N_DEV, 1, n_g), F32),
                    pltpu.VMEM((1, width), F32),
                    pltpu.VMEM((1, q_rank), F32),
                    pltpu.VMEM((1, kv_rank), F32),
                    pltpu.VMEM(w_dkv.shape, BF16),
                    pltpu.VMEM((2, cfg["kdim"], 256), BF16),
                    pltpu.VMEM((2, q_rank, cfg["uq_w"]), BF16),
                    pltpu.VMEM((2, kv_rank, cfg["ukv_w"]), BF16),
                    pltpu.VMEM((tok, cfg["uq_w"]), BF16),
                    pltpu.VMEM((tok, cfg["ukv_w"]), BF16),
                    pltpu.VMEM((2, tok, 256), BF16),
                    pltpu.VMEM((2, tok, 256), BF16),
                    pltpu.SemaphoreType.DMA((n_sems,)),
                    pltpu.SemaphoreType.DMA((n_sems, 4)),
                    pltpu.SemaphoreType.DMA((7,)),
                    pltpu.SemaphoreType.DMA((2,)),
                    pltpu.SemaphoreType.DMA((2,)),
                    pltpu.SemaphoreType.DMA((6,)),
                    pltpu.SemaphoreType.DMA((N_DEV,)),
                    pltpu.SemaphoreType.DMA((N_DEV,)),
                ],
                compiler_params=pltpu.CompilerParams(
                    collective_id=0, has_side_effects=True, vmem_limit_bytes=66_000_000),
                name="mla_block",
            )(tok_blk.reshape(tok, width), gains, wdq, wuq, wdkv, wukv, wo, jnp.asarray(cos2), jnp.asarray(sin2))
            y, c, r = outs[:3]
            return (y.reshape(tok_blk.shape), c.reshape(n_prompts, seq, kv_rank), r.reshape(n_prompts, seq, rope_dim))

        return jax.shard_map(
            local_block,
            mesh=mesh,
            in_specs=(batch_spec, row_spec, mat_spec, row_spec, mat_spec, mat_spec, row_spec, mat_spec, mat_spec),
            out_specs=(batch_spec, batch_spec, batch_spec),
            check_vma=False,
        )(tokens, gain_in, w_dq, gain_q, w_uq, w_dkv, gain_kv, w_ukv, w_out)

    return run_block
```

```python
import functools

import jax
import jax.numpy as jnp
import numpy as np
from jax import lax
from jax.experimental import pallas as pl
from jax.experimental.pallas import tpu as pltpu
from jax.sharding import PartitionSpec as P

EPSILON = 1e-6
ROPE_THETA = 10000.0
MESH = pl.DeviceIdType.MESH
F32 = jnp.float32
BF16 = jnp.bfloat16

RX, RY, RD, RP, RPD = 0, 1, 2, 3, 4

N_DEV = 8
LOOKAHEAD = 3
LAG = 4


def rope_consts(seq_len, rope_dim):
    half = rope_dim // 2
    inv_freq = (ROPE_THETA ** (-2.0 * np.arange(half, dtype=np.float32) / rope_dim)).astype(np.float32)
    angles = np.arange(seq_len, dtype=np.float32)[:, None] * inv_freq[None, :]
    cos_t = np.cos(angles).astype(np.float32)
    sin_t = np.sin(angles).astype(np.float32)
    cos2 = np.concatenate([cos_t, cos_t, cos_t, cos_t], axis=1)
    sin2 = np.concatenate([-sin_t, sin_t, -sin_t, sin_t], axis=1)
    return cos2, sin2


def rope128(v, cos2, sin2):
    lane = lax.broadcasted_iota(jnp.int32, v.shape, 1)
    swapped = jnp.where(lane % 64 < 32, pltpu.roll(v, 96, 1), pltpu.roll(v, 32, 1))
    return v * cos2 + swapped * sin2


def dot(a, b):
    return lax.dot_general(a, b, (((1,), (0,)), ((), ())), preferred_element_type=F32)


def dot_nt(a, b):
    return lax.dot_general(a, b, (((1,), (1,)), ((), ())), preferred_element_type=F32)


def block_kernel(
    cfg,
    x_hbm, gains_hbm, w_dq, w_uq, w_dkv, w_ukv, w_o, cos_hbm, sin_hbm,
    y_hbm, c_hbm, r_hbm, g_dq, g_uq, g_dkv, g_ukv, g_o,
    ao, qd, cq, c_s, r_lo, r_hi, r_out, cos_s, sin_s, gbuf, g1row, gqrow, gkvrow,
    wkv, wbig, wuq, wukv, q4, kv4, acc, xres, yout,
    send_sem, recv_sem, load_sem, x_sem, y_sem, misc_sem, gain_send, gain_recv,
):
    tok = cfg["tok"]
    seq = cfg["seq"]
    width = cfg["width"]
    q_rank = cfg["q_rank"]
    kv_rank = cfg["kv_rank"]
    kdim = cfg["kdim"]
    n_dq, n_u, n_o = cfg["n_dq"], cfg["n_u"], cfg["n_o"]
    dq_w, o_w = cfg["dq_w"], cfg["o_w"]
    uq_w, ukv_w = cfg["uq_w"], cfg["ukv_w"]
    score_scale = cfg["score_scale"]
    first_u = 1 + n_dq
    first_o = first_u + n_u
    n_ticks = first_o + n_o

    me = lax.axis_index("fsdp")
    xn, yn, pt = me ^ 2, me ^ 4, me ^ 1

    def dev(t):
        return (lax.axis_index("dp"), t)

    barrier = pltpu.get_barrier_semaphore()
    for k in range(1, N_DEV):
        pl.semaphore_signal(barrier, inc=1, device_id=dev(me ^ k), device_id_type=MESH)
    pl.semaphore_wait(barrier, N_DEV - 1)

    gain_copies = []
    for k in range(1, N_DEV):
        gain_copies.append(pltpu.make_async_remote_copy(
            src_ref=gains_hbm.at[0], dst_ref=gbuf.at[me], send_sem=gain_send.at[k], recv_sem=gain_recv.at[k],
            device_id=dev(me ^ k), device_id_type=MESH))
        gain_copies[-1].start()

    class Piece:
        def __init__(self, local, full, n, cid, c0, w):
            self.local_ref, self.full, self.n, self.cid = local, full, n, cid
            self.cols = pl.ds(pl.multiple_of(c0, 128), w)

        def local(self):
            return self.local_ref.at[:, self.cols]

        def shard(self, s, half=None):
            r0, nr = (0, self.n) if half is None else (half * (self.n // 2), self.n // 2)
            return self.full.at[pl.ds(pl.multiple_of(s * self.n + r0, 16), nr), self.cols]

        def shards(self, count):
            return self.full.at[pl.ds(0, count * self.n), self.cols]

        def dst(self, buf, slot):
            return buf.at[pl.ds(pl.multiple_of(slot * self.n, 16), self.n), :]

        def remote(self, src, dst, k, t):
            return pltpu.make_async_remote_copy(
                src_ref=src, dst_ref=dst, send_sem=send_sem.at[self.cid], recv_sem=recv_sem.at[self.cid, k],
                device_id=dev(t), device_id_type=MESH)

        def send_own(self):
            for k, t in ((RX, xn), (RY, yn), (RP, pt)):
                self.remote(self.local(), self.shard(me), k, t).start()

        def on_xy(self):
            for h, k, src, other in ((0, RX, xn, yn), (1, RY, yn, xn)):
                s = self.shard(src)
                self.remote(s, s, k, src).wait_recv()
                f = self.shard(src, h)
                self.remote(f, f, RD, other).start()
                self.remote(s, s, RP, pt).start()

        def on_d(self):
            s = self.shard(me ^ 6)
            self.remote(s, s, RD, pt).wait_recv()
            self.remote(s, s, RPD, pt).start()

        def wait_p(self):
            s = self.shards(3)
            self.remote(s, s, RP, pt).wait_recv()

        def wait_pd(self):
            s = self.shards(1)
            self.remote(s, s, RPD, pt).wait_recv()

        def drain(self):
            s = self.shards(7)
            self.remote(s, s, RP, pt).wait_send()

        def load(self, buf, sem, ks, relative=False):
            for k in ks:
                src = self.local() if k == 0 else self.shard(me ^ k)
                pltpu.make_async_copy(src, self.dst(buf, k if relative else me ^ k), sem).start()

    class ColumnPiece(Piece):
        def local(self):
            return self.local_ref

        def shard(self, s, half=None):
            rows = self.full.shape[0]
            r0, nr = (0, rows) if half is None else (half * (rows // 2), rows // 2)
            return self.full.at[pl.ds(r0, nr), pl.ds(pl.multiple_of(s * self.n, 128), self.n)]

        def shards(self, count):
            return self.full.at[:, pl.ds(0, count * self.n)]

        def dst(self, buf, slot):
            return buf.at[:, pl.ds(pl.multiple_of(slot * self.n, 128), self.n)]

    def wait_loaded(ref, sem):
        pltpu.make_async_copy(ref, ref, sem).wait()

    def kv_pieces(_):
        return [ColumnPiece(w_dkv, g_dkv, w_dkv.shape[1], 0, 0, 128)]

    def dq_pieces(c):
        return [Piece(w_dq, g_dq, w_dq.shape[0], 1 + c, c * dq_w, dq_w)]

    def u_pieces(g):
        return [
            Piece(w_ukv, g_ukv, w_ukv.shape[0], first_u + 2 * g, g * ukv_w, ukv_w),
            Piece(w_uq, g_uq, w_uq.shape[0], first_u + 2 * g + 1, g * uq_w, uq_w),
        ]

    def o_pieces(n):
        return [Piece(w_o, g_o, w_o.shape[0], first_u + 2 * n_u + n, n * o_w, o_w)]

    def kv_bufs(_):
        return [(wkv, load_sem.at[4])]

    def dq_bufs(c):
        s = c % 2
        return [(wbig.at[s], load_sem.at[s])]

    def u_bufs(g):
        s = g % 2
        return [(wukv.at[s], load_sem.at[5 + s]), (wuq.at[s], load_sem.at[7 + s])]

    kinds = [
        (0, 1, kv_pieces, kv_bufs),
        (1, n_dq, dq_pieces, dq_bufs),
        (first_u, n_u, u_pieces, u_bufs),
        (first_o, n_o, o_pieces, None),
    ]

    def each_kind(i, fn, which=None):
        for k, (first, count, _, _) in enumerate(kinds if which is None else which):
            @pl.when((i >= first) & (i < first + count))
            def _():
                fn(k, i - first)

    def send_own(k, c):
        for p in kinds[k][2](c):
            p.send_own()

    def on_xy(k, c):
        for p in kinds[k][2](c):
            p.on_xy()

    def on_d(k, c):
        for p in kinds[k][2](c):
            p.on_d()

    def arrive(k, c):
        ps = kinds[k][2](c)
        if cfg["comm"]:
            for p in ps:
                p.wait_p()
                p.wait_pd()
        if cfg["compute"]:
            for p, (buf, sem) in zip(ps, kinds[k][3](c)):
                p.load(buf, sem, range(N_DEV))

    mb = cfg["mb"]
    n_mb = tok // mb
    rows_o = kdim // N_DEV
    heads_dev = rows_o // 128
    near = 6 * rows_o

    def compute_kv(_):
        def body(m, carry):
            rows = pl.ds(pl.multiple_of(m * mb, mb), mb)
            u = dot_nt(ao[rows, 0:width], wkv[...])
            lat = u[:, 0:kv_rank]
            inv = lax.rsqrt(jnp.mean(lat * lat, axis=-1, keepdims=True) + EPSILON)
            c_s[rows, :] = (lat * inv * gkvrow[...]).astype(BF16)
            pe = jnp.concatenate([u[:, kv_rank:], jnp.zeros((mb, 64), F32)], axis=1)
            trows = pl.ds(pl.multiple_of((m * mb) % seq, mb), mb)
            rot = rope128(pe, cos_s[trows, :], sin_s[trows, :])
            r_lo[rows, :] = rot.astype(BF16)
            r_hi[rows, :] = pltpu.roll(rot, 64, 1).astype(BF16)
            r_out[(m * mb) // seq, :, trows] = rot.T[0:64, :].astype(BF16)
            return carry

        lax.fori_loop(0, n_mb, body, 0)
        pltpu.make_async_copy(c_s, c_hbm, misc_sem.at[0]).start()
        pltpu.make_async_copy(r_out, r_hbm, misc_sem.at[1]).start()

    def compute_dq(c):
        slot = c % 2
        cols = pl.ds(pl.multiple_of(c * dq_w, 128), dq_w)

        def body(m, carry):
            rows = pl.ds(pl.multiple_of(m * mb, mb), mb)
            qd[rows, cols] = dot(ao[rows, 0:width], wbig[slot, 0:width, :])
            return carry

        lax.fori_loop(0, n_mb, body, 0)

        @pl.when(c == n_dq - 1)
        def _():
            def norm(m, carry):
                rows = pl.ds(pl.multiple_of(m * 32, 32), 32)
                v = qd[rows, :]
                inv = lax.rsqrt(jnp.mean(v * v, axis=-1, keepdims=True) + EPSILON)
                cq[rows, :] = (v * inv * gqrow[...]).astype(BF16)
                return carry

            lax.fori_loop(0, tok // 32, norm, 0)

    def compute_u(g):
        slot = g % 2

        def proj(m, carry):
            rows = pl.ds(pl.multiple_of(m * mb, mb), mb)
            trows = pl.ds(pl.multiple_of((m * mb) % seq, mb), mb)
            kv4[rows, :] = dot(c_s[rows, :], wukv[slot]).astype(BF16)
            q = dot(cq[rows, :], wuq[slot])
            cos2, sin2 = cos_s[trows, :], sin_s[trows, :]
            lane = lax.broadcasted_iota(jnp.int32, (mb, 128), 1)
            for p in range(uq_w // 384):
                b0 = q[:, 384 * p:384 * p + 128]
                b1 = q[:, 384 * p + 128:384 * p + 256]
                b2 = q[:, 384 * p + 256:384 * p + 384]
                q4[rows, 384 * p:384 * p + 128] = b0.astype(BF16)
                q4[rows, 384 * p + 128:384 * p + 256] = jnp.where(lane < 64, rope128(b1, cos2, sin2), b1).astype(BF16)
                q4[rows, 384 * p + 256:384 * p + 384] = jnp.where(lane < 64, b2, rope128(b2, cos2, sin2)).astype(BF16)
            return carry

        lax.fori_loop(0, n_mb, proj, 0)

        n_pairs = uq_w // 384
        qb_rows = 256

        def attn(t, carry):
            b, p = t // n_pairs, t % n_pairs
            brow = pl.multiple_of(b * seq, seq)
            rows = pl.ds(brow, seq)
            for hh in range(2):
                koff = pl.multiple_of(p * 512 + hh * 256, 128)
                k = kv4[rows, pl.ds(koff, 128)]
                v = kv4[rows, pl.ds(pl.multiple_of(koff + 128, 128), 128)]
                if hh == 0:
                    k_a, k_b = k, r_lo[rows, :]
                else:
                    lane = lax.broadcasted_iota(jnp.int32, (seq, 128), 1)
                    kr = pltpu.roll(k.astype(F32), 64, 1)
                    k_a = jnp.where(lane < 64, 0.0, kr).astype(BF16)
                    k_b = jnp.where(lane < 64, kr, r_hi[rows, :].astype(F32)).astype(BF16)
                kcat = jnp.concatenate([k_a, k_b], axis=1)
                for qb in range(seq // qb_rows):
                    nk = qb_rows * (qb + 1)
                    qrow = pl.ds(pl.multiple_of(brow + qb * qb_rows, qb_rows), qb_rows)
                    q = q4[qrow, pl.ds(pl.multiple_of(p * 384 + hh * 128, 128), 256)]
                    scale = score_scale * 1.4426950408889634
                    row = lax.broadcasted_iota(jnp.int32, (qb_rows, qb_rows), 0)
                    col = lax.broadcasted_iota(jnp.int32, (qb_rows, qb_rows), 1)
                    s = dot_nt(q, kcat[0:nk, :]) * scale
                    parts = [jnp.where(row >= col, s[:, nk - qb_rows:], -1e30)]
                    if qb > 0:
                        parts.insert(0, s[:, :nk - qb_rows])
                    top = functools.reduce(jnp.maximum, [jnp.max(x, axis=-1, keepdims=True) for x in parts])
                    exps = [jnp.exp2(x - top) for x in parts]
                    inv = 1.0 / sum(jnp.sum(x, axis=-1, keepdims=True) for x in exps)
                    probs = [(x * inv).astype(BF16) for x in exps]
                    probs = probs[0] if qb == 0 else jnp.concatenate(probs, axis=1)
                    o = dot(probs, v[0:nk, :])
                    head = g * n_pairs * 2 + p * 2 + hh
                    ocol = pl.multiple_of(((head // heads_dev) ^ me) * rows_o + (head % heads_dev) * 128, 128)
                    ao[qrow, pl.ds(ocol, 128)] = o.astype(BF16)
            return carry

        lax.fori_loop(0, (tok // seq) * n_pairs, attn, 0)

    def y_copy(c, slot):
        return pltpu.make_async_copy(
            yout.at[slot], y_hbm.at[:, pl.ds(pl.multiple_of(c * o_w, 128), o_w)], y_sem.at[slot])

    def o_near(c, carry):
        slot = c % 2
        buf = wbig.at[slot]
        p = o_pieces(c)[0]
        p.load(buf, load_sem.at[slot], (0, 2, 4), relative=True)
        cols = pl.ds(pl.multiple_of(c * o_w, 128), o_w)
        pltpu.make_async_copy(x_hbm.at[:, cols], xres.at[slot], x_sem.at[slot]).start()
        if cfg["comm"]:
            p.wait_p()
        p.load(buf, load_sem.at[slot], (1, 3, 5), relative=True)
        wait_loaded(buf.at[pl.ds(0, near), :], load_sem.at[slot])
        wait_loaded(xres.at[slot], x_sem.at[slot])

        def body(m, carry):
            rows = pl.ds(pl.multiple_of(m * mb, mb), mb)
            acc[c % 3, rows, :] = xres[slot, rows, :].astype(F32) + dot(ao[rows, 0:near], wbig[slot, 0:near, :])
            return carry

        lax.fori_loop(0, n_mb, body, 0)
        return carry

    def o_far(c, carry):
        slot = c % 2
        buf = wbig.at[slot]
        p = o_pieces(c)[0]
        p.load(buf, load_sem.at[2 + slot], (6,), relative=True)
        if cfg["comm"]:
            p.wait_pd()
        p.load(buf, load_sem.at[2 + slot], (7,), relative=True)

        @pl.when(c >= 2)
        def _():
            y_copy(c - 2, slot).wait()

        wait_loaded(buf.at[pl.ds(near, kdim - near), :], load_sem.at[2 + slot])

        def body(m, carry):
            rows = pl.ds(pl.multiple_of(m * mb, mb), mb)
            yout[slot, rows, :] = (
                acc[c % 3, rows, :] + dot(ao[rows, near:kdim], wbig[slot, near:kdim, :])).astype(BF16)
            return carry

        lax.fori_loop(0, n_mb, body, 0)
        y_copy(c, slot).start()
        return carry

    def compute(k, c):
        for (buf, sem) in kinds[k][3](c):
            wait_loaded(buf.at[pl.ds(0, width), :] if k == 1 else buf, sem)
        if k not in cfg["skip"]:
            (compute_kv, compute_dq, compute_u)[k](c)

    LA = cfg["lookahead"]
    for i in range(LA if cfg["comm"] else 0):
        for k, (first, count, _, _) in enumerate(kinds):
            if first <= i < first + count:
                send_own(k, i - first)

    local = [
        pltpu.make_async_copy(gains_hbm.at[0], gbuf.at[me], misc_sem.at[2]),
        pltpu.make_async_copy(cos_hbm, cos_s, misc_sem.at[3]),
        pltpu.make_async_copy(sin_hbm, sin_s, misc_sem.at[4]),
        pltpu.make_async_copy(x_hbm, ao.at[:, pl.ds(0, width)], misc_sem.at[5]),
    ]
    for cp in local:
        cp.start()
    for cp in local:
        cp.wait()
    for k in range(1, N_DEV):
        gain_copies[k - 1].wait()

    n1, nq, nkv = width // N_DEV, q_rank // N_DEV, kv_rank // N_DEV
    for j in range(N_DEV):
        g1row[:, n1 * j:n1 * (j + 1)] = gbuf[j, :, 0:n1]
    gqrow[...] = jnp.concatenate([gbuf[j, :, n1:n1 + nq] for j in range(N_DEV)], axis=1)
    gkvrow[...] = jnp.concatenate([gbuf[j, :, n1 + nq:n1 + nq + nkv] for j in range(N_DEV)], axis=1)

    if cfg["compute"]:
        def norm_x(m, carry):
            rows = pl.ds(pl.multiple_of(m * 16, 16), 16)
            v = ao[rows, 0:width].astype(F32)
            inv = lax.rsqrt(jnp.mean(v * v, axis=-1, keepdims=True) + EPSILON)
            ao[rows, 0:width] = (v * inv * g1row[...]).astype(BF16)
            return carry

        lax.fori_loop(0, tok // 16, norm_x, 0)

    def each_early(i, fn):
        each_kind(i, fn, kinds[:3])

    def near_done(n):
        return jnp.clip(jnp.minimum(n + 1, 2 * (n - LAG + 1)), 0, n_o)

    def far_done(n):
        return jnp.clip(jnp.minimum(n - 1, near_done(n)), 0, n_o)

    def tick(i, carry):
        if cfg["comm"]:
            each_kind(i, on_xy)
            each_kind(i + LA, send_own)
            each_kind(i - 2, on_d)
        each_early(i - 3, arrive)
        if cfg["compute"]:
            each_early(i - LAG, compute)
            if 3 not in cfg["skip"]:
                n = i - first_o
                lax.fori_loop(near_done(n - 1), near_done(n), o_near, 0)
                lax.fori_loop(far_done(n - 1), far_done(n), o_far, 0)
        return carry

    lax.fori_loop(0, n_ticks + 2, tick, 0)

    def drain(i, carry):
        each_kind(i, lambda k, c: [p.drain() for p in kinds[k][2](c)])
        return carry

    if cfg["comm"]:
        lax.fori_loop(0, n_ticks, drain, 0)
    if cfg["compute"]:
        if 0 not in cfg["skip"]: pltpu.make_async_copy(c_s, c_hbm, misc_sem.at[0]).wait()
        if 0 not in cfg["skip"]: pltpu.make_async_copy(r_out, r_hbm, misc_sem.at[1]).wait()
        if 3 not in cfg["skip"]: y_copy(n_o - 2, (n_o - 2) % 2).wait()
        if 3 not in cfg["skip"]: y_copy(n_o - 1, (n_o - 1) % 2).wait()


def copy_out_kernel(steps, y_in, c_in, r_in, y_out, c_out, r_out, y_buf, c_buf, r_buf, sem_in, sem_out):
    n = y_in.shape[0] // steps
    chunks = [(y_in.at[pl.ds(i * n, n)], y_buf.at[pl.ds(i * n, n)], y_out.at[pl.ds(i * n, n)]) for i in range(steps)]
    chunks += [(c_in, c_buf, c_out), (r_in, r_buf, r_out)]
    for i, (src, buf, _) in enumerate(chunks):
        pltpu.make_async_copy(src, buf, sem_in.at[i]).start()
    for i, (src, buf, dst) in enumerate(chunks):
        pltpu.make_async_copy(src, buf, sem_in.at[i]).wait()
        pltpu.make_async_copy(buf, dst, sem_out.at[i]).start()
    for i, (_, buf, dst) in enumerate(chunks):
        pltpu.make_async_copy(buf, dst, sem_out.at[i]).wait()


def copy_out(y, c, r):
    steps = 16
    any_spec = pl.BlockSpec(memory_space=pl.ANY)
    return pl.pallas_call(
        functools.partial(copy_out_kernel, steps),
        out_shape=[jax.ShapeDtypeStruct(v.shape, v.dtype) for v in (y, c, r)],
        in_specs=[any_spec] * 3,
        out_specs=[any_spec] * 3,
        scratch_shapes=[pltpu.VMEM(v.shape, v.dtype) for v in (y, c, r)]
        + [pltpu.SemaphoreType.DMA((steps + 2,)), pltpu.SemaphoreType.DMA((steps + 2,))],
        compiler_params=pltpu.CompilerParams(vmem_limit_bytes=60_000_000),
        name="copy_out",
    )(y, c, r)


def solution(mesh, compute=True, comm=True, lookahead=LOOKAHEAD, skip=()):
    batch_spec = P(("dp", "fsdp"))
    row_spec = P("fsdp")
    mat_spec = P("fsdp", None)

    def run_block(tokens, gain_in, w_dq, gain_q, w_uq, w_dkv, gain_kv, w_ukv, w_out):
        seq = tokens.shape[1]
        rope_dim = w_dkv.shape[1] - gain_kv.shape[0]
        nope_total = w_ukv.shape[1] - w_out.shape[0]
        n_heads = (w_uq.shape[1] - nope_total) // rope_dim
        cos2, sin2 = rope_consts(seq, rope_dim)

        def local_block(tok_blk, g1, wdq, gq, wuq, wdkv, gkv, wukv, wo):
            n_prompts, _, width = tok_blk.shape
            tok = n_prompts * seq
            q_rank, kv_rank = gain_q.shape[0], gain_kv.shape[0]
            heads_per = 4
            cfg = dict(
                tok=tok, seq=seq, width=width, q_rank=q_rank, kv_rank=kv_rank, kdim=w_out.shape[0],
                n_dq=q_rank // 256, n_u=n_heads // heads_per, n_o=width // 256, dq_w=256, o_w=256,
                uq_w=heads_per * (w_uq.shape[1] // n_heads), ukv_w=heads_per * (w_ukv.shape[1] // n_heads),
                score_scale=(w_uq.shape[1] // n_heads) ** -0.5, mb=256, compute=compute, comm=comm, lookahead=lookahead, skip=skip,
            )
            n_sems = 1 + cfg["n_dq"] + 2 * cfg["n_u"] + cfg["n_o"]
            n_g = g1.shape[0] + gq.shape[0] + gkv.shape[0]
            gains = jnp.concatenate([g1, gq, gkv]).astype(F32).reshape(1, 1, n_g)
            any_spec = pl.BlockSpec(memory_space=pl.ANY)
            outs = pl.pallas_call(
                functools.partial(block_kernel, cfg),
                out_shape=[
                    jax.ShapeDtypeStruct((tok, width), BF16),
                    jax.ShapeDtypeStruct((tok, kv_rank), BF16),
                    jax.ShapeDtypeStruct((n_prompts, rope_dim, seq), BF16),
                    jax.ShapeDtypeStruct(w_dq.shape, BF16),
                    jax.ShapeDtypeStruct(w_uq.shape, BF16),
                    jax.ShapeDtypeStruct(w_dkv.shape[::-1], BF16),
                    jax.ShapeDtypeStruct(w_ukv.shape, BF16),
                    jax.ShapeDtypeStruct(w_out.shape, BF16),
                ],
                in_specs=[any_spec] * 9,
                out_specs=[any_spec] * 8,
                scratch_shapes=[
                    pltpu.VMEM((tok, cfg["kdim"]), BF16),
                    pltpu.VMEM((tok, q_rank), F32),
                    pltpu.VMEM((tok, q_rank), BF16),
                    pltpu.VMEM((tok, kv_rank), BF16),
                    pltpu.VMEM((tok, 128), BF16),
                    pltpu.VMEM((tok, 128), BF16),
                    pltpu.VMEM((n_prompts, rope_dim, seq), BF16),
                    pltpu.VMEM((seq, 128), F32),
                    pltpu.VMEM((seq, 128), F32),
                    pltpu.VMEM((N_DEV, 1, n_g), F32),
                    pltpu.VMEM((1, width), F32),
                    pltpu.VMEM((1, q_rank), F32),
                    pltpu.VMEM((1, kv_rank), F32),
                    pltpu.VMEM(w_dkv.shape[::-1], BF16),
                    pltpu.VMEM((2, cfg["kdim"], 256), BF16),
                    pltpu.VMEM((2, q_rank, cfg["uq_w"]), BF16),
                    pltpu.VMEM((2, kv_rank, cfg["ukv_w"]), BF16),
                    pltpu.VMEM((tok, cfg["uq_w"]), BF16),
                    pltpu.VMEM((tok, cfg["ukv_w"]), BF16),
                    pltpu.VMEM((3, tok, 256), F32),
                    pltpu.VMEM((2, tok, 256), BF16),
                    pltpu.VMEM((2, tok, 256), BF16),
                    pltpu.SemaphoreType.DMA((n_sems,)),
                    pltpu.SemaphoreType.DMA((n_sems, 5)),
                    pltpu.SemaphoreType.DMA((9,)),
                    pltpu.SemaphoreType.DMA((2,)),
                    pltpu.SemaphoreType.DMA((2,)),
                    pltpu.SemaphoreType.DMA((6,)),
                    pltpu.SemaphoreType.DMA((N_DEV,)),
                    pltpu.SemaphoreType.DMA((N_DEV,)),
                ],
                compiler_params=pltpu.CompilerParams(
                    collective_id=0, has_side_effects=True, vmem_limit_bytes=66_000_000),
                name="mla_block",
            )(tok_blk.reshape(tok, width), gains, wdq, wuq, wdkv.T, wukv, wo, jnp.asarray(cos2), jnp.asarray(sin2))
            y, c, r = copy_out(*outs[:3])
            return (y.reshape(tok_blk.shape), c.reshape(n_prompts, seq, kv_rank), jnp.swapaxes(r, 1, 2))

        return jax.shard_map(
            local_block,
            mesh=mesh,
            in_specs=(batch_spec, row_spec, mat_spec, row_spec, mat_spec, mat_spec, row_spec, mat_spec, mat_spec),
            out_specs=(batch_spec, batch_spec, batch_spec),
            check_vma=False,
        )(tokens, gain_in, w_dq, gain_q, w_uq, w_dkv, gain_kv, w_ukv, w_out)

    return run_block
```

```python
import functools

import jax
import jax.numpy as jnp
import numpy as np
from jax import lax
from jax.experimental import pallas as pl
from jax.experimental.pallas import tpu as pltpu
from jax.sharding import PartitionSpec as P

EPSILON = 1e-6
ROPE_THETA = 10000.0
MESH = pl.DeviceIdType.MESH
F32 = jnp.float32
BF16 = jnp.bfloat16

RX, RY, RD, RP, RPD = 0, 1, 2, 3, 4

N_DEV = 8
LOOKAHEAD = 3
LAG = 4
K1_VMEM = 50_600_000
COPY_VMEM = 20_000_000


def rope_consts(seq_len, rope_dim):
    half = rope_dim // 2
    inv_freq = (ROPE_THETA ** (-2.0 * np.arange(half, dtype=np.float32) / rope_dim)).astype(np.float32)
    angles = np.arange(seq_len, dtype=np.float32)[:, None] * inv_freq[None, :]
    cos_t = np.cos(angles).astype(np.float32)
    sin_t = np.sin(angles).astype(np.float32)
    cos2 = np.concatenate([cos_t, cos_t, cos_t, cos_t], axis=1)
    sin2 = np.concatenate([-sin_t, sin_t, -sin_t, sin_t], axis=1)
    return cos2, sin2


def rope128(v, cos2, sin2):
    lane = lax.broadcasted_iota(jnp.int32, v.shape, 1)
    swapped = jnp.where(lane % 64 < 32, pltpu.roll(v, 96, 1), pltpu.roll(v, 32, 1))
    return v * cos2 + swapped * sin2


def dot(a, b):
    return lax.dot_general(a, b, (((1,), (0,)), ((), ())), preferred_element_type=F32)


def dot_nt(a, b):
    return lax.dot_general(a, b, (((1,), (1,)), ((), ())), preferred_element_type=F32)


def block_kernel(
    cfg,
    x_hbm, gains_hbm, w_dq, w_uq, w_dkv, w_ukv, w_o, cos_hbm, sin_hbm,
    y_v, c_s, r_out, g_dq, g_uq, g_dkv, g_ukv, g_o,
    ao, qd, cq, r_lo, r_hi, cos_s, sin_s, gbuf, g1row, gqrow, gkvrow,
    wbig, wuq, wukv, q4, kv4, xres,
    send_sem, recv_sem, load_sem, x_sem, misc_sem, gain_send, gain_recv,
):
    tok = cfg["tok"]
    seq = cfg["seq"]
    width = cfg["width"]
    q_rank = cfg["q_rank"]
    kv_rank = cfg["kv_rank"]
    kdim = cfg["kdim"]
    n_dq, n_u, n_o = cfg["n_dq"], cfg["n_u"], cfg["n_o"]
    dq_w, o_w = cfg["dq_w"], cfg["o_w"]
    uq_w, ukv_w = cfg["uq_w"], cfg["ukv_w"]
    score_scale = cfg["score_scale"]
    first_u = 1 + n_dq
    first_o = first_u + n_u
    n_ticks = first_o + n_o

    me = lax.axis_index("fsdp")
    xn, yn, pt = me ^ 2, me ^ 4, me ^ 1

    def dev(t):
        return (lax.axis_index("dp"), t)

    barrier = pltpu.get_barrier_semaphore()
    for k in range(1, N_DEV):
        pl.semaphore_signal(barrier, inc=1, device_id=dev(me ^ k), device_id_type=MESH)
    pl.semaphore_wait(barrier, N_DEV - 1)

    gain_copies = []
    for k in range(1, N_DEV):
        gain_copies.append(pltpu.make_async_remote_copy(
            src_ref=gains_hbm, dst_ref=gbuf.at[me], send_sem=gain_send.at[k], recv_sem=gain_recv.at[k],
            device_id=dev(me ^ k), device_id_type=MESH))
        gain_copies[-1].start()

    class Piece:
        def __init__(self, local, full, n, cid, c0, w):
            self.local_ref, self.full, self.n, self.cid = local, full, n, cid
            self.cols = pl.ds(pl.multiple_of(c0, 128), w)

        def local(self):
            return self.local_ref.at[:, self.cols]

        def shard(self, s, half=None):
            r0, nr = (0, self.n) if half is None else (half * (self.n // 2), self.n // 2)
            return self.full.at[pl.ds(pl.multiple_of(s * self.n + r0, 16), nr), self.cols]

        def shards(self, count):
            return self.full.at[pl.ds(0, count * self.n), self.cols]

        def dst(self, buf, slot):
            return buf.at[pl.ds(pl.multiple_of(slot * self.n, 16), self.n), :]

        def remote(self, src, dst, k, t):
            return pltpu.make_async_remote_copy(
                src_ref=src, dst_ref=dst, send_sem=send_sem.at[self.cid], recv_sem=recv_sem.at[self.cid, k],
                device_id=dev(t), device_id_type=MESH)

        def send_own(self):
            for k, t in ((RX, xn), (RY, yn), (RP, pt)):
                self.remote(self.local(), self.shard(me), k, t).start()

        def on_xy(self):
            for h, k, src, other in ((0, RX, xn, yn), (1, RY, yn, xn)):
                s = self.shard(src)
                self.remote(s, s, k, src).wait_recv()
                f = self.shard(src, h)
                self.remote(f, f, RD, other).start()
                self.remote(s, s, RP, pt).start()

        def on_d(self):
            s = self.shard(me ^ 6)
            self.remote(s, s, RD, pt).wait_recv()
            self.remote(s, s, RPD, pt).start()

        def wait_p(self):
            s = self.shards(3)
            self.remote(s, s, RP, pt).wait_recv()

        def wait_pd(self):
            s = self.shards(1)
            self.remote(s, s, RPD, pt).wait_recv()

        def drain(self):
            s = self.shards(7)
            self.remote(s, s, RP, pt).wait_send()

        def load(self, buf, sem, ks, relative=False):
            for k in ks:
                src = self.local() if k == 0 else self.shard(me ^ k)
                pltpu.make_async_copy(src, self.dst(buf, k if relative else me ^ k), sem).start()

    class ColumnPiece(Piece):
        def local(self):
            return self.local_ref

        def shard(self, s, half=None):
            rows = self.full.shape[0]
            r0, nr = (0, rows) if half is None else (half * (rows // 2), rows // 2)
            return self.full.at[pl.ds(r0, nr), pl.ds(pl.multiple_of(s * self.n, 128), self.n)]

        def shards(self, count):
            return self.full.at[:, pl.ds(0, count * self.n)]

        def dst(self, buf, slot):
            return buf.at[:, pl.ds(pl.multiple_of(slot * self.n, 128), self.n)]

    def wait_loaded(ref, sem):
        pltpu.make_async_copy(ref, ref, sem).wait()

    def kv_pieces(_):
        return [ColumnPiece(w_dkv, g_dkv, w_dkv.shape[1], 0, 0, 128)]

    def dq_pieces(c):
        return [Piece(w_dq, g_dq, w_dq.shape[0], 1 + c, c * dq_w, dq_w)]

    def u_pieces(g):
        return [
            Piece(w_ukv, g_ukv, w_ukv.shape[0], first_u + 2 * g, g * ukv_w, ukv_w),
            Piece(w_uq, g_uq, w_uq.shape[0], first_u + 2 * g + 1, g * uq_w, uq_w),
        ]

    def o_pieces(n):
        return [Piece(w_o, g_o, w_o.shape[0], first_u + 2 * n_u + n, n * o_w, o_w)]

    wkv = y_v.at[pl.ds(0, w_dkv.shape[0]), :]

    def kv_bufs(_):
        return [(wkv, load_sem.at[4])]

    def dq_bufs(c):
        s = c % 2
        return [(wbig.at[s], load_sem.at[s])]

    def u_bufs(g):
        s = g % 2
        return [(wukv.at[s], load_sem.at[5 + s]), (wuq.at[s], load_sem.at[7 + s])]

    kinds = [
        (0, 1, kv_pieces, kv_bufs),
        (1, n_dq, dq_pieces, dq_bufs),
        (first_u, n_u, u_pieces, u_bufs),
        (first_o, n_o, o_pieces, None),
    ]

    def each_kind(i, fn, which=None):
        for k, (first, count, _, _) in enumerate(kinds if which is None else which):
            @pl.when((i >= first) & (i < first + count))
            def _():
                fn(k, i - first)

    def send_own(k, c):
        for p in kinds[k][2](c):
            p.send_own()

    def on_xy(k, c):
        for p in kinds[k][2](c):
            p.on_xy()

    def on_d(k, c):
        for p in kinds[k][2](c):
            p.on_d()

    def arrive(k, c):
        ps = kinds[k][2](c)
        if cfg["comm"]:
            for p in ps:
                p.wait_p()
                p.wait_pd()
        if cfg["compute"]:
            for p, (buf, sem) in zip(ps, kinds[k][3](c)):
                p.load(buf, sem, range(N_DEV))

    mb = cfg["mb"]
    n_mb = tok // mb
    rows_o = kdim // N_DEV
    heads_dev = rows_o // 128
    near = 6 * rows_o

    def compute_kv(_):
        def body(m, carry):
            rows = pl.ds(pl.multiple_of(m * mb, mb), mb)
            u = dot_nt(ao[rows, 0:width], wkv[...])
            lat = u[:, 0:kv_rank]
            inv = lax.rsqrt(jnp.mean(lat * lat, axis=-1, keepdims=True) + EPSILON)
            c_s[rows, :] = (lat * inv * gkvrow[...]).astype(BF16)
            pe = jnp.concatenate([u[:, kv_rank:], jnp.zeros((mb, 64), F32)], axis=1)
            trows = pl.ds(pl.multiple_of((m * mb) % seq, mb), mb)
            rot = rope128(pe, cos_s[trows, :], sin_s[trows, :])
            r_lo[rows, :] = rot.astype(BF16)
            r_hi[rows, :] = pltpu.roll(rot, 64, 1).astype(BF16)
            r_out[(m * mb) // seq, :, trows] = rot.T[0:64, :].astype(BF16)
            return carry

        lax.fori_loop(0, n_mb, body, 0)

    def compute_dq(c):
        slot = c % 2

        def body(m, carry):
            rows = pl.ds(pl.multiple_of(m * mb, mb), mb)
            qd[c, rows, :] = dot(ao[rows, 0:width], wbig[slot, 0:width, :])
            return carry

        lax.fori_loop(0, n_mb, body, 0)

        @pl.when(c == n_dq - 1)
        def _():
            def norm(m, carry):
                rows = pl.ds(pl.multiple_of(m * 32, 32), 32)
                vs = [qd[j, rows, :] for j in range(n_dq)]
                mean = sum(jnp.sum(v * v, axis=-1, keepdims=True) for v in vs) * (1.0 / q_rank)
                inv = lax.rsqrt(mean + EPSILON)
                for j, v in enumerate(vs):
                    cols = slice(dq_w * j, dq_w * (j + 1))
                    cq[rows, cols] = (v * inv * gqrow[:, cols]).astype(BF16)
                return carry

            lax.fori_loop(0, tok // 32, norm, 0)

    def compute_u(g):
        slot = g % 2

        def proj(m, carry):
            rows = pl.ds(pl.multiple_of(m * mb, mb), mb)
            trows = pl.ds(pl.multiple_of((m * mb) % seq, mb), mb)
            kv4[rows, :] = dot(c_s[rows, :], wukv[slot]).astype(BF16)
            q = dot(cq[rows, :], wuq[slot])
            cos2, sin2 = cos_s[trows, :], sin_s[trows, :]
            lane = lax.broadcasted_iota(jnp.int32, (mb, 128), 1)
            for p in range(uq_w // 384):
                b0 = q[:, 384 * p:384 * p + 128]
                b1 = q[:, 384 * p + 128:384 * p + 256]
                b2 = q[:, 384 * p + 256:384 * p + 384]
                q4[rows, 384 * p:384 * p + 128] = b0.astype(BF16)
                q4[rows, 384 * p + 128:384 * p + 256] = jnp.where(lane < 64, rope128(b1, cos2, sin2), b1).astype(BF16)
                q4[rows, 384 * p + 256:384 * p + 384] = jnp.where(lane < 64, b2, rope128(b2, cos2, sin2)).astype(BF16)
            return carry

        lax.fori_loop(0, n_mb, proj, 0)

        n_pairs = uq_w // 384
        qb_rows = 256

        def attn(t, carry):
            b, p = t // n_pairs, t % n_pairs
            brow = pl.multiple_of(b * seq, seq)
            rows = pl.ds(brow, seq)
            for hh in range(2):
                koff = pl.multiple_of(p * 512 + hh * 256, 128)
                k = kv4[rows, pl.ds(koff, 128)]
                v = kv4[rows, pl.ds(pl.multiple_of(koff + 128, 128), 128)]
                if hh == 0:
                    k_a, k_b = k, r_lo[rows, :]
                else:
                    lane = lax.broadcasted_iota(jnp.int32, (seq, 128), 1)
                    kr = pltpu.roll(k.astype(F32), 64, 1)
                    k_a = jnp.where(lane < 64, 0.0, kr).astype(BF16)
                    k_b = jnp.where(lane < 64, kr, r_hi[rows, :].astype(F32)).astype(BF16)
                kcat = jnp.concatenate([k_a, k_b], axis=1)
                for qb in range(seq // qb_rows):
                    nk = qb_rows * (qb + 1)
                    qrow = pl.ds(pl.multiple_of(brow + qb * qb_rows, qb_rows), qb_rows)
                    q = q4[qrow, pl.ds(pl.multiple_of(p * 384 + hh * 128, 128), 256)]
                    scale = score_scale * 1.4426950408889634
                    row = lax.broadcasted_iota(jnp.int32, (qb_rows, qb_rows), 0)
                    col = lax.broadcasted_iota(jnp.int32, (qb_rows, qb_rows), 1)
                    s = dot_nt(q, kcat[0:nk, :]) * scale
                    parts = [jnp.where(row >= col, s[:, nk - qb_rows:], -1e30)]
                    if qb > 0:
                        parts.insert(0, s[:, :nk - qb_rows])
                    top = functools.reduce(jnp.maximum, [jnp.max(x, axis=-1, keepdims=True) for x in parts])
                    exps = [jnp.exp2(x - top) for x in parts]
                    inv = 1.0 / sum(jnp.sum(x, axis=-1, keepdims=True) for x in exps)
                    probs = [(x * inv).astype(BF16) for x in exps]
                    probs = probs[0] if qb == 0 else jnp.concatenate(probs, axis=1)
                    o = dot(probs, v[0:nk, :])
                    head = g * n_pairs * 2 + p * 2 + hh
                    ocol = pl.multiple_of(((head // heads_dev) ^ me) * rows_o + (head % heads_dev) * 128, 128)
                    ao[qrow, pl.ds(ocol, 128)] = o.astype(BF16)
            return carry

        lax.fori_loop(0, (tok // seq) * n_pairs, attn, 0)

    def o_near(c, carry):
        slot = c % 2
        buf = wbig.at[slot]
        p = o_pieces(c)[0]
        p.load(buf, load_sem.at[slot], (0, 2, 4), relative=True)
        cols = pl.ds(pl.multiple_of(c * o_w, 128), o_w)
        pltpu.make_async_copy(x_hbm.at[:, cols], xres, x_sem).start()
        if cfg["comm"]:
            p.wait_p()
        p.load(buf, load_sem.at[slot], (1, 3, 5), relative=True)
        wait_loaded(buf.at[pl.ds(0, near), :], load_sem.at[slot])
        wait_loaded(xres, x_sem)

        def body(m, carry):
            rows = pl.ds(pl.multiple_of(m * mb, mb), mb)
            qd[c % 3, rows, :] = xres[rows, :].astype(F32) + dot(ao[rows, 0:near], wbig[slot, 0:near, :])
            return carry

        if cfg["mm"]:
            lax.fori_loop(0, n_mb, body, 0)
        return carry

    def o_far(c, carry):
        slot = c % 2
        buf = wbig.at[slot]
        p = o_pieces(c)[0]
        cols = pl.ds(pl.multiple_of(c * o_w, 128), o_w)
        p.load(buf, load_sem.at[2 + slot], (6,), relative=True)
        if cfg["comm"]:
            p.wait_pd()
        p.load(buf, load_sem.at[2 + slot], (7,), relative=True)
        wait_loaded(buf.at[pl.ds(near, kdim - near), :], load_sem.at[2 + slot])

        def body(m, carry):
            rows = pl.ds(pl.multiple_of(m * mb, mb), mb)
            y_v[rows, cols] = (
                qd[c % 3, rows, :] + dot(ao[rows, near:kdim], wbig[slot, near:kdim, :])).astype(BF16)
            return carry

        if cfg["mm"]:
            lax.fori_loop(0, n_mb, body, 0)
        return carry

    def compute(k, c):
        for (buf, sem) in kinds[k][3](c):
            wait_loaded(buf.at[pl.ds(0, width), :] if k == 1 else buf, sem)
        if k not in cfg["skip"]:
            (compute_kv, compute_dq, compute_u)[k](c)

    LA = cfg["lookahead"]
    for i in range(LA if cfg["comm"] else 0):
        for k, (first, count, _, _) in enumerate(kinds):
            if first <= i < first + count:
                send_own(k, i - first)

    local = [
        pltpu.make_async_copy(gains_hbm, gbuf.at[me], misc_sem.at[2]),
        pltpu.make_async_copy(cos_hbm, cos_s, misc_sem.at[3]),
        pltpu.make_async_copy(sin_hbm, sin_s, misc_sem.at[4]),
        pltpu.make_async_copy(x_hbm, ao.at[:, pl.ds(0, width)], misc_sem.at[5]),
    ]
    for cp in local:
        cp.start()
    for cp in local:
        cp.wait()
    for k in range(1, N_DEV):
        gain_copies[k - 1].wait()

    gq_parts, gkv_parts = [], []
    for j in range(N_DEV):
        for t in range(7):
            g1row[:, 896 * j + 128 * t:896 * j + 128 * (t + 1)] = gbuf[j, t:t + 1, :]
        gq_parts += [gbuf[j, 7:8, :], gbuf[j, 8:9, 0:64]]
        gkv_parts += [gbuf[j, 8:9, 64:128]]
    gqrow[...] = jnp.concatenate(gq_parts, axis=1)
    gkvrow[...] = jnp.concatenate(gkv_parts, axis=1)

    if cfg["compute"]:
        def norm_x(m, carry):
            rows = pl.ds(pl.multiple_of(m * 16, 16), 16)
            v = ao[rows, 0:width].astype(F32)
            inv = lax.rsqrt(jnp.mean(v * v, axis=-1, keepdims=True) + EPSILON)
            ao[rows, 0:width] = (v * inv * g1row[...]).astype(BF16)
            return carry

        lax.fori_loop(0, tok // 16, norm_x, 0)

    def each_early(i, fn):
        each_kind(i, fn, kinds[:3])

    def near_done(n):
        return jnp.clip(jnp.minimum(n + 1, 2 * (n - LAG)), 0, n_o)

    def far_done(n):
        return jnp.clip(jnp.minimum(n - 1, near_done(n)), 0, n_o)

    def tick(i, carry):
        if cfg["comm"]:
            each_kind(i, on_xy)
            each_kind(i + LA, send_own)
        n = i - first_o
        if cfg["compute"] and 3 not in cfg["skip"]:
            lax.fori_loop(near_done(n - 1), near_done(n), o_near, 0)
        if cfg["comm"]:
            each_kind(i - 2, on_d)
        each_early(i - 3, arrive)
        if cfg["compute"]:
            each_early(i - LAG, compute)
            if 3 not in cfg["skip"]:
                lax.fori_loop(far_done(n - 1), far_done(n), o_far, 0)
        return carry

    lax.fori_loop(0, n_ticks + 2, tick, 0)

    def drain(i, carry):
        each_kind(i, lambda k, c: [p.drain() for p in kinds[k][2](c)])
        return carry

    if cfg["comm"]:
        lax.fori_loop(0, n_ticks, drain, 0)
    if cfg["compute"]:
        pass


def copy_out_kernel(steps, y_v, c_v, r_v, y_out, c_out, r_out, sem):
    n = y_v.shape[0] // steps
    copies = [(y_v.at[pl.ds(i * n, n)], y_out.at[pl.ds(i * n, n)]) for i in range(steps)]
    copies = [
        pltpu.make_async_copy(src, dst, sem.at[i])
        for i, (src, dst) in enumerate(copies + [(c_v, c_out), (r_v, r_out)])]
    for cp in copies:
        cp.start()
    for cp in copies:
        cp.wait()


def copy_out(y, c, r):
    steps = 8
    return pl.pallas_call(
        functools.partial(copy_out_kernel, steps),
        out_shape=[jax.ShapeDtypeStruct(v.shape, v.dtype) for v in (y, c, r)],
        in_specs=[pl.BlockSpec(memory_space=pltpu.VMEM)] * 3,
        out_specs=[pl.BlockSpec(memory_space=pl.ANY)] * 3,
        scratch_shapes=[pltpu.SemaphoreType.DMA((steps + 2,))],
        compiler_params=pltpu.CompilerParams(vmem_limit_bytes=COPY_VMEM),
        name="copy_out",
    )(y, c, r)


def solution(mesh, compute=True, comm=True, lookahead=LOOKAHEAD, skip=(), mm=True):
    batch_spec = P(("dp", "fsdp"))
    row_spec = P("fsdp")
    mat_spec = P("fsdp", None)

    def run_block(tokens, gain_in, w_dq, gain_q, w_uq, w_dkv, gain_kv, w_ukv, w_out):
        seq = tokens.shape[1]
        rope_dim = w_dkv.shape[1] - gain_kv.shape[0]
        nope_total = w_ukv.shape[1] - w_out.shape[0]
        n_heads = (w_uq.shape[1] - nope_total) // rope_dim
        cos2, sin2 = rope_consts(seq, rope_dim)

        def local_block(tok_blk, g1, wdq, gq, wuq, wdkv, gkv, wukv, wo):
            n_prompts, _, width = tok_blk.shape
            tok = n_prompts * seq
            q_rank, kv_rank = gain_q.shape[0], gain_kv.shape[0]
            heads_per = 4
            cfg = dict(
                tok=tok, seq=seq, width=width, q_rank=q_rank, kv_rank=kv_rank, kdim=w_out.shape[0],
                n_dq=q_rank // 256, n_u=n_heads // heads_per, n_o=width // 256, dq_w=256, o_w=256,
                uq_w=heads_per * (w_uq.shape[1] // n_heads), ukv_w=heads_per * (w_ukv.shape[1] // n_heads),
                score_scale=(w_uq.shape[1] // n_heads) ** -0.5, mb=256, compute=compute, comm=comm, lookahead=lookahead, skip=skip, mm=mm,
            )
            n_sems = 1 + cfg["n_dq"] + 2 * cfg["n_u"] + cfg["n_o"]
            n1, nq, nkv = g1.shape[0], gq.shape[0], gkv.shape[0]
            gains = (
                jnp.pad(g1.astype(F32), (0, nq + nkv)) + jnp.pad(gq.astype(F32), (n1, nkv))
                + jnp.pad(gkv.astype(F32), (n1 + nq, 0))).reshape(9, 128)
            any_spec = pl.BlockSpec(memory_space=pl.ANY)
            outs = pl.pallas_call(
                functools.partial(block_kernel, cfg),
                out_shape=[
                    pltpu.VMEM((tok, width), BF16),
                    pltpu.VMEM((tok, kv_rank), BF16),
                    pltpu.VMEM((n_prompts, rope_dim, seq), BF16),
                    jax.ShapeDtypeStruct(w_dq.shape, BF16),
                    jax.ShapeDtypeStruct(w_uq.shape, BF16),
                    jax.ShapeDtypeStruct(w_dkv.shape[::-1], BF16),
                    jax.ShapeDtypeStruct(w_ukv.shape, BF16),
                    jax.ShapeDtypeStruct(w_out.shape, BF16),
                ],
                in_specs=[any_spec] * 9,
                out_specs=[pl.BlockSpec(memory_space=pltpu.VMEM)] * 3 + [any_spec] * 5,
                scratch_shapes=[
                    pltpu.VMEM((tok, cfg["kdim"]), BF16),
                    pltpu.VMEM((cfg["n_dq"], tok, 256), F32),
                    pltpu.VMEM((tok, q_rank), BF16),
                    pltpu.VMEM((tok, 128), BF16),
                    pltpu.VMEM((tok, 128), BF16),
                    pltpu.VMEM((seq, 128), F32),
                    pltpu.VMEM((seq, 128), F32),
                    pltpu.VMEM((N_DEV, 9, 128), F32),
                    pltpu.VMEM((1, width), F32),
                    pltpu.VMEM((1, q_rank), F32),
                    pltpu.VMEM((1, kv_rank), F32),
                    pltpu.VMEM((2, cfg["kdim"], 256), BF16),
                    pltpu.VMEM((2, q_rank, cfg["uq_w"]), BF16),
                    pltpu.VMEM((2, kv_rank, cfg["ukv_w"]), BF16),
                    pltpu.VMEM((tok, cfg["uq_w"]), BF16),
                    pltpu.VMEM((tok, cfg["ukv_w"]), BF16),
                    pltpu.VMEM((tok, 256), BF16),
                    pltpu.SemaphoreType.DMA((n_sems,)),
                    pltpu.SemaphoreType.DMA((n_sems, 5)),
                    pltpu.SemaphoreType.DMA((9,)),
                    pltpu.SemaphoreType.DMA,
                    pltpu.SemaphoreType.DMA((6,)),
                    pltpu.SemaphoreType.DMA((N_DEV,)),
                    pltpu.SemaphoreType.DMA((N_DEV,)),
                ],
                compiler_params=pltpu.CompilerParams(
                    collective_id=0, has_side_effects=True, vmem_limit_bytes=K1_VMEM),
                name="mla_block",
            )(tok_blk.reshape(tok, width), gains, wdq, wuq, wdkv.T, wukv, wo, jnp.asarray(cos2), jnp.asarray(sin2))
            y, c, r = copy_out(*outs[:3])
            return (y.reshape(tok_blk.shape), c.reshape(n_prompts, seq, kv_rank), jnp.swapaxes(r, 1, 2))

        return jax.shard_map(
            local_block,
            mesh=mesh,
            in_specs=(batch_spec, row_spec, mat_spec, row_spec, mat_spec, mat_spec, row_spec, mat_spec, mat_spec),
            out_specs=(batch_spec, batch_spec, batch_spec),
            check_vma=False,
        )(tokens, gain_in, w_dq, gain_q, w_uq, w_dkv, gain_kv, w_ukv, w_out)

    return run_block
```

```python
import functools

import jax
import jax.numpy as jnp
import numpy as np
from jax import lax
from jax.experimental import pallas as pl
from jax.experimental.pallas import tpu as pltpu
from jax.sharding import PartitionSpec as P

EPSILON = 1e-6
ROPE_THETA = 10000.0
MESH = pl.DeviceIdType.MESH
F32 = jnp.float32
BF16 = jnp.bfloat16

RX, RY, RD, RP, RPD = 0, 1, 2, 3, 4

N_DEV = 8
LOOKAHEAD = 3
LAG = 4
DRAIN_LAG = 6
K1_VMEM = 51_100_000
COPY_VMEM = 20_000_000


def rope_consts(seq_len, rope_dim):
    half = rope_dim // 2
    inv_freq = (ROPE_THETA ** (-2.0 * np.arange(half, dtype=np.float32) / rope_dim)).astype(np.float32)
    angles = np.arange(seq_len, dtype=np.float32)[:, None] * inv_freq[None, :]
    cos_t = np.cos(angles).astype(np.float32)
    sin_t = np.sin(angles).astype(np.float32)
    cos2 = np.concatenate([cos_t, cos_t, cos_t, cos_t], axis=1)
    sin2 = np.concatenate([-sin_t, sin_t, -sin_t, sin_t], axis=1)
    return cos2, sin2


def rope128(v, cos2, sin2):
    lane = lax.broadcasted_iota(jnp.int32, v.shape, 1)
    swapped = jnp.where(lane % 64 < 32, pltpu.roll(v, 96, 1), pltpu.roll(v, 32, 1))
    return v * cos2 + swapped * sin2


def dot(a, b):
    return lax.dot_general(a, b, (((1,), (0,)), ((), ())), preferred_element_type=F32)


def dot_nt(a, b):
    return lax.dot_general(a, b, (((1,), (1,)), ((), ())), preferred_element_type=F32)


def block_kernel(
    cfg,
    x_hbm, gains_hbm, w_dq, w_uq, w_dkv, w_ukv, w_o, cos_hbm, sin_hbm,
    y_v, c_s, r_out, g_dq, g_uq, g_dkv, g_ukv, g_o,
    ao, qd, cq, r_lo, r_hi, cos_s, sin_s, gbuf, g1row, gqrow, gkvrow,
    wbig, wuq, wukv, q4, kv4, xres,
    send_sem, recv_sem, load_sem, x_sem, misc_sem, gain_send, gain_recv,
):
    tok = cfg["tok"]
    seq = cfg["seq"]
    width = cfg["width"]
    q_rank = cfg["q_rank"]
    kv_rank = cfg["kv_rank"]
    kdim = cfg["kdim"]
    n_dq, n_u, n_o = cfg["n_dq"], cfg["n_u"], cfg["n_o"]
    dq_w, o_w = cfg["dq_w"], cfg["o_w"]
    uq_w, ukv_w = cfg["uq_w"], cfg["ukv_w"]
    score_scale = cfg["score_scale"]
    first_u = 1 + n_dq
    first_o = first_u + n_u
    n_ticks = first_o + n_o

    me = lax.axis_index("fsdp")
    xn, yn, pt = me ^ 2, me ^ 4, me ^ 1

    def dev(t):
        return (lax.axis_index("dp"), t)

    barrier = pltpu.get_barrier_semaphore()
    for k in range(1, N_DEV):
        pl.semaphore_signal(barrier, inc=1, device_id=dev(me ^ k), device_id_type=MESH)
    pl.semaphore_wait(barrier, N_DEV - 1)

    gain_copies = []
    for k in range(1, N_DEV):
        gain_copies.append(pltpu.make_async_remote_copy(
            src_ref=gains_hbm, dst_ref=gbuf.at[me], send_sem=gain_send.at[k], recv_sem=gain_recv.at[k],
            device_id=dev(me ^ k), device_id_type=MESH))
        gain_copies[-1].start()

    class Piece:
        def __init__(self, local, full, n, cid, c0, w):
            self.local_ref, self.full, self.n, self.cid = local, full, n, cid
            self.cols = pl.ds(pl.multiple_of(c0, 128), w)

        def local(self):
            return self.local_ref.at[:, self.cols]

        def shard(self, s, half=None):
            r0, nr = (0, self.n) if half is None else (half * (self.n // 2), self.n // 2)
            return self.full.at[pl.ds(pl.multiple_of(s * self.n + r0, 16), nr), self.cols]

        def shards(self, count):
            return self.full.at[pl.ds(0, count * self.n), self.cols]

        def dst(self, buf, slot):
            return buf.at[pl.ds(pl.multiple_of(slot * self.n, 16), self.n), :]

        def remote(self, src, dst, k, t):
            return pltpu.make_async_remote_copy(
                src_ref=src, dst_ref=dst, send_sem=send_sem.at[self.cid], recv_sem=recv_sem.at[self.cid, k],
                device_id=dev(t), device_id_type=MESH)

        def send_own(self):
            for k, t in ((RX, xn), (RY, yn), (RP, pt)):
                self.remote(self.local(), self.shard(me), k, t).start()

        def on_xy(self):
            for h, k, src, other in ((0, RX, xn, yn), (1, RY, yn, xn)):
                s = self.shard(src)
                self.remote(s, s, k, src).wait_recv()
                f = self.shard(src, h)
                self.remote(f, f, RD, other).start()
                self.remote(s, s, RP, pt).start()

        def on_d(self):
            s = self.shard(me ^ 6)
            self.remote(s, s, RD, pt).wait_recv()
            self.remote(s, s, RPD, pt).start()

        def wait_p(self):
            s = self.shards(3)
            self.remote(s, s, RP, pt).wait_recv()

        def wait_pd(self):
            s = self.shards(1)
            self.remote(s, s, RPD, pt).wait_recv()

        def drain(self):
            s = self.shards(7)
            self.remote(s, s, RP, pt).wait_send()

        def load(self, buf, sem, ks, relative=False):
            for k in ks:
                src = self.local() if k == 0 else self.shard(me ^ k)
                pltpu.make_async_copy(src, self.dst(buf, k if relative else me ^ k), sem).start()

    class ColumnPiece(Piece):
        def local(self):
            return self.local_ref

        def shard(self, s, half=None):
            rows = self.full.shape[0]
            r0, nr = (0, rows) if half is None else (half * (rows // 2), rows // 2)
            return self.full.at[pl.ds(r0, nr), pl.ds(pl.multiple_of(s * self.n, 128), self.n)]

        def shards(self, count):
            return self.full.at[:, pl.ds(0, count * self.n)]

        def dst(self, buf, slot):
            return buf.at[:, pl.ds(pl.multiple_of(slot * self.n, 128), self.n)]

    def wait_loaded(ref, sem):
        pltpu.make_async_copy(ref, ref, sem).wait()

    def kv_pieces(_):
        return [ColumnPiece(w_dkv, g_dkv, w_dkv.shape[1], 0, 0, 128)]

    def dq_pieces(c):
        return [Piece(w_dq, g_dq, w_dq.shape[0], 1 + c, c * dq_w, dq_w)]

    def u_pieces(g):
        return [
            Piece(w_ukv, g_ukv, w_ukv.shape[0], first_u + 2 * g, g * ukv_w, ukv_w),
            Piece(w_uq, g_uq, w_uq.shape[0], first_u + 2 * g + 1, g * uq_w, uq_w),
        ]

    def o_pieces(n):
        return [Piece(w_o, g_o, w_o.shape[0], first_u + 2 * n_u + n, n * o_w, o_w)]

    wkv = y_v.at[pl.ds(0, w_dkv.shape[0]), :]

    def kv_bufs(_):
        return [(wkv, load_sem.at[4])]

    def dq_bufs(c):
        s = c % 2
        return [(wbig.at[s], load_sem.at[s])]

    def u_bufs(g):
        s = g % 2
        return [(wukv.at[s], load_sem.at[5 + s]), (wuq.at[s], load_sem.at[7 + s])]

    kinds = [
        (0, 1, kv_pieces, kv_bufs),
        (1, n_dq, dq_pieces, dq_bufs),
        (first_u, n_u, u_pieces, u_bufs),
        (first_o, n_o, o_pieces, None),
    ]

    def each_kind(i, fn, which=None):
        for k, (first, count, _, _) in enumerate(kinds if which is None else which):
            @pl.when((i >= first) & (i < first + count))
            def _():
                fn(k, i - first)

    def send_own(k, c):
        for p in kinds[k][2](c):
            p.send_own()

    def on_xy(k, c):
        for p in kinds[k][2](c):
            p.on_xy()

    def on_d(k, c):
        for p in kinds[k][2](c):
            p.on_d()

    def drain(k, c):
        for p in kinds[k][2](c):
            p.drain()

    def arrive(k, c):
        ps = kinds[k][2](c)
        for p in ps:
            p.wait_p()
            p.wait_pd()
        for p, (buf, sem) in zip(ps, kinds[k][3](c)):
            p.load(buf, sem, range(N_DEV))

    mb = cfg["mb"]
    n_mb = tok // mb
    rows_o = kdim // N_DEV
    heads_dev = rows_o // 128
    near = 6 * rows_o

    def compute_kv(_):
        def body(m, carry):
            rows = pl.ds(pl.multiple_of(m * mb, mb), mb)
            u = dot_nt(ao[rows, 0:width], wkv[...])
            lat = u[:, 0:kv_rank]
            inv = lax.rsqrt(jnp.mean(lat * lat, axis=-1, keepdims=True) + EPSILON)
            c_s[rows, :] = (lat * inv * gkvrow[...]).astype(BF16)
            pe = jnp.concatenate([u[:, kv_rank:], jnp.zeros((mb, 64), F32)], axis=1)
            trows = pl.ds(pl.multiple_of((m * mb) % seq, mb), mb)
            rot = rope128(pe, cos_s[trows, :], sin_s[trows, :])
            r_lo[rows, :] = rot.astype(BF16)
            r_hi[rows, :] = pltpu.roll(rot, 64, 1).astype(BF16)
            r_out[(m * mb) // seq, :, trows] = rot.T[0:64, :].astype(BF16)
            return carry

        lax.fori_loop(0, n_mb, body, 0)

    def compute_dq(c):
        slot = c % 2

        def body(m, carry):
            rows = pl.ds(pl.multiple_of(m * mb, mb), mb)
            qd[c, rows, :] = dot(ao[rows, 0:width], wbig[slot, 0:width, :])
            return carry

        lax.fori_loop(0, n_mb, body, 0)

        @pl.when(c == n_dq - 1)
        def _():
            def norm(m, carry):
                rows = pl.ds(pl.multiple_of(m * 32, 32), 32)
                vs = [qd[j, rows, :] for j in range(n_dq)]
                mean = sum(jnp.sum(v * v, axis=-1, keepdims=True) for v in vs) * (1.0 / q_rank)
                inv = lax.rsqrt(mean + EPSILON)
                for j, v in enumerate(vs):
                    cols = slice(dq_w * j, dq_w * (j + 1))
                    cq[rows, cols] = (v * inv * gqrow[:, cols]).astype(BF16)
                return carry

            lax.fori_loop(0, tok // 32, norm, 0)

    def compute_u(g):
        slot = g % 2

        def proj(m, carry):
            rows = pl.ds(pl.multiple_of(m * mb, mb), mb)
            trows = pl.ds(pl.multiple_of((m * mb) % seq, mb), mb)
            kv4[rows, :] = dot(c_s[rows, :], wukv[slot]).astype(BF16)
            q = dot(cq[rows, :], wuq[slot])
            cos2, sin2 = cos_s[trows, :], sin_s[trows, :]
            lane = lax.broadcasted_iota(jnp.int32, (mb, 128), 1)
            for p in range(uq_w // 384):
                b0 = q[:, 384 * p:384 * p + 128]
                b1 = q[:, 384 * p + 128:384 * p + 256]
                b2 = q[:, 384 * p + 256:384 * p + 384]
                q4[rows, 384 * p:384 * p + 128] = b0.astype(BF16)
                q4[rows, 384 * p + 128:384 * p + 256] = jnp.where(lane < 64, rope128(b1, cos2, sin2), b1).astype(BF16)
                q4[rows, 384 * p + 256:384 * p + 384] = jnp.where(lane < 64, b2, rope128(b2, cos2, sin2)).astype(BF16)
            return carry

        lax.fori_loop(0, n_mb, proj, 0)

        n_pairs = uq_w // 384
        qb_rows = 256

        def attn(t, carry):
            b, p = t // n_pairs, t % n_pairs
            brow = pl.multiple_of(b * seq, seq)
            rows = pl.ds(brow, seq)
            for hh in range(2):
                koff = pl.multiple_of(p * 512 + hh * 256, 128)
                k = kv4[rows, pl.ds(koff, 128)]
                v = kv4[rows, pl.ds(pl.multiple_of(koff + 128, 128), 128)]
                if hh == 0:
                    k_a, k_b = k, r_lo[rows, :]
                else:
                    lane = lax.broadcasted_iota(jnp.int32, (seq, 128), 1)
                    kr = pltpu.roll(k.astype(F32), 64, 1)
                    k_a = jnp.where(lane < 64, 0.0, kr).astype(BF16)
                    k_b = jnp.where(lane < 64, kr, r_hi[rows, :].astype(F32)).astype(BF16)
                kcat = jnp.concatenate([k_a, k_b], axis=1)
                for qb in range(seq // qb_rows):
                    nk = qb_rows * (qb + 1)
                    qrow = pl.ds(pl.multiple_of(brow + qb * qb_rows, qb_rows), qb_rows)
                    q = q4[qrow, pl.ds(pl.multiple_of(p * 384 + hh * 128, 128), 256)]
                    scale = score_scale * 1.4426950408889634
                    row = lax.broadcasted_iota(jnp.int32, (qb_rows, qb_rows), 0)
                    col = lax.broadcasted_iota(jnp.int32, (qb_rows, qb_rows), 1)
                    s = dot_nt(q, kcat[0:nk, :]) * scale
                    parts = [jnp.where(row >= col, s[:, nk - qb_rows:], -1e30)]
                    if qb > 0:
                        parts.insert(0, s[:, :nk - qb_rows])
                    top = functools.reduce(jnp.maximum, [jnp.max(x, axis=-1, keepdims=True) for x in parts])
                    exps = [jnp.exp2(x - top) for x in parts]
                    inv = 1.0 / sum(jnp.sum(x, axis=-1, keepdims=True) for x in exps)
                    probs = [(x * inv).astype(BF16) for x in exps]
                    probs = probs[0] if qb == 0 else jnp.concatenate(probs, axis=1)
                    o = dot(probs, v[0:nk, :])
                    head = g * n_pairs * 2 + p * 2 + hh
                    ocol = pl.multiple_of(((head // heads_dev) ^ me) * rows_o + (head % heads_dev) * 128, 128)
                    ao[qrow, pl.ds(ocol, 128)] = o.astype(BF16)
            return carry

        lax.fori_loop(0, (tok // seq) * n_pairs, attn, 0)

    def near_rows(slot):
        return wbig.at[slot].at[pl.ds(0, near), :]

    def far_rows(slot):
        return wbig.at[slot].at[pl.ds(near, kdim - near), :]

    def near_load(c, carry):
        slot = c % 2
        p = o_pieces(c)[0]
        p.load(wbig.at[slot], load_sem.at[slot], (0, 2, 4), relative=True)
        pltpu.make_async_copy(
            x_hbm.at[:, pl.ds(pl.multiple_of(c * o_w, 128), o_w)], xres.at[slot], x_sem.at[slot]).start()
        p.wait_p()
        p.load(wbig.at[slot], load_sem.at[slot], (1, 3, 5), relative=True)
        return carry

    def near_sum(c, carry):
        slot = c % 2
        wait_loaded(near_rows(slot), load_sem.at[slot])
        wait_loaded(xres.at[slot], x_sem.at[slot])

        def body(m, carry):
            rows = pl.ds(pl.multiple_of(m * mb, mb), mb)
            qd[c % n_dq, rows, :] = xres[slot, rows, :].astype(F32) + dot(ao[rows, 0:near], wbig[slot, 0:near, :])
            return carry

        return lax.fori_loop(0, n_mb, body, carry)

    def far_load(c, carry):
        slot = c % 2
        p = o_pieces(c)[0]
        p.load(wbig.at[slot], load_sem.at[2 + slot], (6,), relative=True)
        p.wait_pd()
        p.load(wbig.at[slot], load_sem.at[2 + slot], (7,), relative=True)
        return carry

    def far_sum(c, carry):
        slot = c % 2
        cols = pl.ds(pl.multiple_of(c * o_w, 128), o_w)
        wait_loaded(far_rows(slot), load_sem.at[2 + slot])

        def body(m, carry):
            rows = pl.ds(pl.multiple_of(m * mb, mb), mb)
            y_v[rows, cols] = (
                qd[c % n_dq, rows, :] + dot(ao[rows, near:kdim], wbig[slot, near:kdim, :])).astype(BF16)
            return carry

        return lax.fori_loop(0, n_mb, body, carry)

    def compute(k, c):
        for (buf, sem) in kinds[k][3](c):
            wait_loaded(buf.at[pl.ds(0, width), :] if k == 1 else buf, sem)
        (compute_kv, compute_dq, compute_u)[k](c)

    for i in range(LOOKAHEAD):
        for k, (first, count, _, _) in enumerate(kinds):
            if first <= i < first + count:
                send_own(k, i - first)

    local = [
        pltpu.make_async_copy(gains_hbm, gbuf.at[me], misc_sem.at[2]),
        pltpu.make_async_copy(cos_hbm, cos_s, misc_sem.at[3]),
        pltpu.make_async_copy(sin_hbm, sin_s, misc_sem.at[4]),
        pltpu.make_async_copy(x_hbm, ao.at[:, pl.ds(0, width)], misc_sem.at[5]),
    ]
    for cp in local:
        cp.start()
    for cp in local:
        cp.wait()
    for k in range(1, N_DEV):
        gain_copies[k - 1].wait()

    gq_parts, gkv_parts = [], []
    for j in range(N_DEV):
        for t in range(7):
            g1row[:, 896 * j + 128 * t:896 * j + 128 * (t + 1)] = gbuf[j, t:t + 1, :]
        gq_parts += [gbuf[j, 7:8, :], gbuf[j, 8:9, 0:64]]
        gkv_parts += [gbuf[j, 8:9, 64:128]]
    gqrow[...] = jnp.concatenate(gq_parts, axis=1)
    gkvrow[...] = jnp.concatenate(gkv_parts, axis=1)

    def norm_x(m, carry):
        rows = pl.ds(pl.multiple_of(m * 16, 16), 16)
        v = ao[rows, 0:width].astype(F32)
        inv = lax.rsqrt(jnp.mean(v * v, axis=-1, keepdims=True) + EPSILON)
        ao[rows, 0:width] = (v * inv * g1row[...]).astype(BF16)
        return carry

    lax.fori_loop(0, tok // 16, norm_x, 0)

    def each_early(i, fn):
        each_kind(i, fn, kinds[:3])

    def near_done(n):
        return jnp.clip(jnp.minimum(n + 1, 2 * (n - LAG)), 0, n_o)

    def far_done(n):
        return jnp.clip(jnp.minimum(n - 1, near_done(n)), 0, n_o)

    def tick(i, carry):
        each_kind(i, on_xy)
        each_kind(i + LOOKAHEAD, send_own)
        n = i - first_o
        for fn in (near_load, near_sum):
            lax.fori_loop(near_done(n - 1), near_done(n), fn, 0)
        each_kind(i - 2, on_d)
        lax.fori_loop(far_done(n - 2), far_done(n - 1), far_sum, 0)
        lax.fori_loop(far_done(n - 1), far_done(n), far_load, 0)
        each_kind(i - DRAIN_LAG, drain)
        each_early(i - 3, arrive)
        each_early(i - LAG, compute)
        return carry

    lax.fori_loop(0, n_ticks + 3, tick, 0)

    def finish(i, carry):
        each_kind(i, drain)
        return carry

    lax.fori_loop(n_ticks + 3 - DRAIN_LAG, n_ticks, finish, 0)


def copy_out_kernel(steps, y_v, c_v, r_v, y_out, c_out, r_out, sem):
    n = y_v.shape[0] // steps
    copies = [(y_v.at[pl.ds(i * n, n)], y_out.at[pl.ds(i * n, n)]) for i in range(steps)]
    copies = [
        pltpu.make_async_copy(src, dst, sem.at[i])
        for i, (src, dst) in enumerate(copies + [(c_v, c_out), (r_v, r_out)])]
    for cp in copies:
        cp.start()
    for cp in copies:
        cp.wait()


def copy_out(y, c, r):
    steps = 8
    return pl.pallas_call(
        functools.partial(copy_out_kernel, steps),
        out_shape=[jax.ShapeDtypeStruct(v.shape, v.dtype) for v in (y, c, r)],
        in_specs=[pl.BlockSpec(memory_space=pltpu.VMEM)] * 3,
        out_specs=[pl.BlockSpec(memory_space=pl.ANY)] * 3,
        scratch_shapes=[pltpu.SemaphoreType.DMA((steps + 2,))],
        compiler_params=pltpu.CompilerParams(vmem_limit_bytes=COPY_VMEM),
        name="copy_out",
    )(y, c, r)


def solution(mesh):
    batch_spec = P(("dp", "fsdp"))
    row_spec = P("fsdp")
    mat_spec = P("fsdp", None)

    def run_block(tokens, gain_in, w_dq, gain_q, w_uq, w_dkv, gain_kv, w_ukv, w_out):
        seq = tokens.shape[1]
        rope_dim = w_dkv.shape[1] - gain_kv.shape[0]
        nope_total = w_ukv.shape[1] - w_out.shape[0]
        n_heads = (w_uq.shape[1] - nope_total) // rope_dim
        cos2, sin2 = rope_consts(seq, rope_dim)

        def local_block(tok_blk, g1, wdq, gq, wuq, wdkv, gkv, wukv, wo):
            n_prompts, _, width = tok_blk.shape
            tok = n_prompts * seq
            q_rank, kv_rank = gain_q.shape[0], gain_kv.shape[0]
            heads_per = 4
            cfg = dict(
                tok=tok, seq=seq, width=width, q_rank=q_rank, kv_rank=kv_rank, kdim=w_out.shape[0],
                n_dq=q_rank // 256, n_u=n_heads // heads_per, n_o=width // 256, dq_w=256, o_w=256,
                uq_w=heads_per * (w_uq.shape[1] // n_heads), ukv_w=heads_per * (w_ukv.shape[1] // n_heads),
                score_scale=(w_uq.shape[1] // n_heads) ** -0.5, mb=256,
            )
            n_sems = 1 + cfg["n_dq"] + 2 * cfg["n_u"] + cfg["n_o"]
            n1, nq, nkv = g1.shape[0], gq.shape[0], gkv.shape[0]
            gains = (
                jnp.pad(g1.astype(F32), (0, nq + nkv)) + jnp.pad(gq.astype(F32), (n1, nkv))
                + jnp.pad(gkv.astype(F32), (n1 + nq, 0))).reshape(9, 128)
            any_spec = pl.BlockSpec(memory_space=pl.ANY)
            outs = pl.pallas_call(
                functools.partial(block_kernel, cfg),
                out_shape=[
                    pltpu.VMEM((tok, width), BF16),
                    pltpu.VMEM((tok, kv_rank), BF16),
                    pltpu.VMEM((n_prompts, rope_dim, seq), BF16),
                    jax.ShapeDtypeStruct(w_dq.shape, BF16),
                    jax.ShapeDtypeStruct(w_uq.shape, BF16),
                    jax.ShapeDtypeStruct(w_dkv.shape[::-1], BF16),
                    jax.ShapeDtypeStruct(w_ukv.shape, BF16),
                    jax.ShapeDtypeStruct(w_out.shape, BF16),
                ],
                in_specs=[any_spec] * 9,
                out_specs=[pl.BlockSpec(memory_space=pltpu.VMEM)] * 3 + [any_spec] * 5,
                scratch_shapes=[
                    pltpu.VMEM((tok, cfg["kdim"]), BF16),
                    pltpu.VMEM((cfg["n_dq"], tok, 256), F32),
                    pltpu.VMEM((tok, q_rank), BF16),
                    pltpu.VMEM((tok, 128), BF16),
                    pltpu.VMEM((tok, 128), BF16),
                    pltpu.VMEM((seq, 128), F32),
                    pltpu.VMEM((seq, 128), F32),
                    pltpu.VMEM((N_DEV, 9, 128), F32),
                    pltpu.VMEM((1, width), F32),
                    pltpu.VMEM((1, q_rank), F32),
                    pltpu.VMEM((1, kv_rank), F32),
                    pltpu.VMEM((2, cfg["kdim"], 256), BF16),
                    pltpu.VMEM((2, q_rank, cfg["uq_w"]), BF16),
                    pltpu.VMEM((2, kv_rank, cfg["ukv_w"]), BF16),
                    pltpu.VMEM((tok, cfg["uq_w"]), BF16),
                    pltpu.VMEM((tok, cfg["ukv_w"]), BF16),
                    pltpu.VMEM((2, tok, 256), BF16),
                    pltpu.SemaphoreType.DMA((n_sems,)),
                    pltpu.SemaphoreType.DMA((n_sems, 5)),
                    pltpu.SemaphoreType.DMA((9,)),
                    pltpu.SemaphoreType.DMA((2,)),
                    pltpu.SemaphoreType.DMA((6,)),
                    pltpu.SemaphoreType.DMA((N_DEV,)),
                    pltpu.SemaphoreType.DMA((N_DEV,)),
                ],
                compiler_params=pltpu.CompilerParams(
                    collective_id=0, has_side_effects=True, vmem_limit_bytes=K1_VMEM),
                name="mla_block",
            )(tok_blk.reshape(tok, width), gains, wdq, wuq, wdkv.T, wukv, wo, jnp.asarray(cos2), jnp.asarray(sin2))
            y, c, r = copy_out(*outs[:3])
            return (y.reshape(tok_blk.shape), c.reshape(n_prompts, seq, kv_rank), jnp.swapaxes(r, 1, 2))

        return jax.shard_map(
            local_block,
            mesh=mesh,
            in_specs=(batch_spec, row_spec, mat_spec, row_spec, mat_spec, mat_spec, row_spec, mat_spec, mat_spec),
            out_specs=(batch_spec, batch_spec, batch_spec),
            check_vma=False,
        )(tokens, gain_in, w_dq, gain_q, w_uq, w_dkv, gain_kv, w_ukv, w_out)

    return run_block
```
